32 devices in a mesh: gx: 2 (over core), gy: 16 (over z, y, x).
Axes of the slice: x: 2, y: 2, z: 4, core: 2. Of those that a mesh axis runs over, the one named last changes fastest.
Arguments:
- echoes: bfloat16 [32, 256, 16, 200], P('gx', 'gy'), may hold values from -6 to 6
- start: float32 [200, 32], replicated, may hold values from -6 to 6
- ranks: int32 [2, 16, 1], P('gx', 'gy'), may hold values from 2 to 32
- counts: int32 [2, 16, 1], P('gx', 'gy'), may hold values from 1 to 4
Outputs:
- filtered: bfloat16 [32, 256, 16, 200], P('gx', 'gy')
The draws below stay inside these ranges and needn't reach their ends.
All inputs are finite; a program needn't handle non-finite values.
Results may differ from the reference program's by a relative error of at most 0.0075.
Values may be sent and summed in bfloat16 or wider, within the bound.
A program may use at most 128 MiB of HBM per device.

```python
import jax
import jax.numpy as jnp
from jax import lax

BS = 16
BZ = 16
NZ = 16
F = 200
K = 32
ITERS = 4
NX = 32
NY = 256
NBZ = 1


def touch_ends(values, own_key, least, largest):
    longest = values.shape.index(max(values.shape))
    spots = []
    for shift in (0, 1):
        where = [jax.random.randint(jax.random.fold_in(own_key, axis), (), 0, length) for axis, length in enumerate(values.shape)]
        where[longest] = (where[longest] + shift) % values.shape[longest]
        spots.append(tuple(where))
    return values.at[spots[0]].set(least).at[spots[1]].set(largest)


def level_of(rng, shape, shards, smallest, high):
    def one(dim, blocks):
        heights = jax.random.uniform(jax.random.fold_in(jax.random.fold_in(rng, 6), dim), (blocks,), jnp.float32, smallest / len(shards), high / len(shards))
        return jnp.repeat(jnp.exp(heights), shape[dim] // blocks).reshape((-1,) + (1,) * (len(shape) - dim - 1))

    factor_of = one(*shards[0])
    for cut in shards[1:]:
        factor_of = factor_of * one(*cut)
    return factor_of


def noise(key, extent, scale, most, pieces=(), kind=jnp.bfloat16):
    array = scale * jax.random.normal(key, extent, jnp.float32)
    if pieces:
        array = array * level_of(key, extent, pieces, -0.22, 0.18)
    return jnp.clip(array, -most, most).astype(kind)


def setup_inputs(seed: int = 0) -> dict:
    key_of = jax.random.split(jax.random.key(seed), 5)
    return {
        "echoes": noise(key_of[0], (NX, NY, NZ, F), 1.0, 6.0, ((0, 2), (1, 16))),
        "start": noise(key_of[1], (F, K), 1.0, 6.0, (), jnp.float32),
        "ranks": touch_ends(jax.random.randint(key_of[2], (NX // BS, NY // BS, NBZ), 2, K + 1), jax.random.fold_in(key_of[2], 1), 2, K).astype(jnp.int32),
        "counts": touch_ends(jax.random.randint(key_of[3], (NX // BS, NY // BS, NBZ), 1, ITERS + 1), jax.random.fold_in(key_of[3], 1), 1, ITERS).astype(jnp.int32),
    }


def tent(offset, span):
    inside = (offset >= 0.0) & (offset < span)
    return jnp.where(inside, 1.0 + jnp.minimum(offset, span - 1.0 - offset), 0.0).astype(jnp.float32)

def segment_grams(region):
    sizex, sizey, depth, frames = region.shape
    half = BZ // 2
    parts = region.reshape(sizex, sizey, depth // half, half, frames).astype(jnp.float32)
    return jnp.einsum('xyshf,xyshg->sfg', parts, parts, precision=lax.Precision.HIGHEST)

def subspace(grams, start, counts):
    basis = jnp.broadcast_to(start, (grams.shape[0],) + start.shape)
    for turn in range(ITERS):
        moved = jnp.einsum('sfg,sgk->sfk', grams, basis, precision=lax.Precision.HIGHEST)
        inner = jnp.einsum('sfk,sfl->skl', moved, moved, precision=lax.Precision.HIGHEST)
        factor = jnp.linalg.cholesky(inner)
        solved = lax.linalg.triangular_solve(factor, moved, left_side=False, lower=True, transpose_a=True)
        basis = jnp.where((turn < counts)[:, None, None], solved, basis)
    return basis

def filter_column(region, segments, ranks, counts, start):
    sizex, sizey, depth, frames = region.shape
    half = BZ // 2
    grams = (segments[:-1] + segments[1:]) / float(sizex * sizey * BZ)
    basis = subspace(grams, start, counts)
    keep = (jnp.arange(K)[None, :] < ranks[:, None]).astype(jnp.float32)
    vectors_all = (basis * keep[:, None, :]).astype(jnp.bfloat16)
    weight = tent(jnp.arange(sizex, dtype=jnp.float32), float(sizex))[:, None, None, None] * tent(jnp.arange(sizey, dtype=jnp.float32), float(sizey))[None, :, None, None] * tent(jnp.arange(BZ, dtype=jnp.float32), float(BZ))[None, None, :, None]

    def add_block(index, total):
        offset = (jnp.asarray(index).astype(jnp.int32) * half).astype(jnp.int32)
        block = lax.dynamic_slice_in_dim(region, offset, BZ, 2)
        vectors = vectors_all[index].astype(jnp.float32)
        coeff = jnp.einsum('xyzf,fk->xyzk', block.astype(jnp.float32), vectors, precision=lax.Precision.HIGHEST).astype(jnp.bfloat16)
        clutter = jnp.einsum('xyzk,fk->xyzf', coeff.astype(jnp.float32), vectors, precision=lax.Precision.HIGHEST)
        contrib = weight * (block.astype(jnp.float32) - clutter)
        previous = lax.dynamic_slice_in_dim(total, offset, BZ, 2)
        return lax.dynamic_update_slice_in_dim(total, previous + contrib, offset, 2)
    return lax.fori_loop(0, grams.shape[0], add_block, jnp.zeros(region.shape, jnp.float32))

def reference(echoes, start, ranks, counts):
    sizex, sizey, depth, frames = echoes.shape
    grid_x = sizex // BS
    grid_y = sizey // BS
    columns = grid_y - 1
    zero = jnp.zeros((), jnp.int32)

    def visit(index, total):
        index = jnp.asarray(index).astype(jnp.int32)
        blockx = index // columns
        blocky = index % columns
        anchor = (blockx * BS, blocky * BS, zero, zero)
        region = lax.dynamic_slice(echoes, anchor, (2 * BS, 2 * BS, depth, frames))
        part = filter_column(region, segment_grams(region), ranks[blockx, blocky], counts[blockx, blocky], start)
        previous = lax.dynamic_slice(total, anchor, part.shape)
        return lax.dynamic_update_slice(total, previous + part, anchor)
    total = lax.fori_loop(0, (grid_x - 1) * columns, visit, jnp.zeros(echoes.shape, jnp.float32))
    span = float(2 * BS)
    posx = jnp.arange(sizex, dtype=jnp.float32)
    posy = jnp.arange(sizey, dtype=jnp.float32)
    posz = jnp.arange(depth, dtype=jnp.float32)
    coverx = jnp.sum(tent(posx[None, :] - BS * jnp.arange(grid_x - 1, dtype=jnp.float32)[:, None], span), axis=0)
    covery = jnp.sum(tent(posy[None, :] - BS * jnp.arange(grid_y - 1, dtype=jnp.float32)[:, None], span), axis=0)
    nblocks = 2 * depth // BZ - 1
    coverz = jnp.sum(tent(posz[None, :] - BZ // 2 * jnp.arange(nblocks, dtype=jnp.float32)[:, None], float(BZ)), axis=0)
    cover = coverx[:, None, None, None] * covery[None, :, None, None] * coverz[None, None, :, None]
    return (total / cover).astype(jnp.bfloat16)
```

```python
import functools

import jax
import jax.numpy as jnp
from jax import lax
from jax.experimental import pallas as pl
from jax.experimental.pallas import tpu as pltpu
from jax.sharding import PartitionSpec as P

BZ = 16
ITERS = 4
LANES = 128
SUB = 8
GRANT = 16 << 20
MESH = pl.DeviceIdType.MESH


def tent(offset, span):
    inside = (offset >= 0.0) & (offset < span)
    return jnp.where(inside, 1.0 + jnp.minimum(offset, span - 1.0 - offset), 0.0)


def padded(size):
    return -(-size // LANES) * LANES


def row_of(tile, k):
    return jnp.broadcast_to(tile[k : k + 1, :], tile.shape)


def halves(x):
    high = x.astype(jnp.bfloat16)
    return high, (x - high.astype(jnp.float32)).astype(jnp.bfloat16)


def nt(a, b):
    return lax.dot_general(a, b, (((1,), (1,)), ((), ())), preferred_element_type=jnp.float32)


def orthonormal_rows(moved):
    size, width = moved.shape
    tiles = size // SUB
    high, low = halves(moved)
    inner = nt(high, high) + nt(low, high) + nt(high, low)
    columns = []
    for j in range(size):
        first = j // SUB
        columns.append(
            [
                jnp.broadcast_to(inner[SUB * i : SUB * i + SUB, j : j + 1], (SUB, LANES))
                for i in range(first, tiles)
            ]
        )
    rows = [
        [moved[SUB * i : SUB * i + SUB, LANES * h : LANES * h + LANES] for h in range(width // LANES)]
        for i in range(tiles)
    ]
    place = lax.broadcasted_iota(jnp.int32, (SUB, LANES), 0)
    scales = [None] * tiles
    for k in range(size):
        own, at = k // SUB, k % SUB
        root = lax.rsqrt(row_of(columns[k][0], at))
        scales[own] = root if at == 0 else jnp.where(place == at, root, scales[own])
        if k == size - 1:
            break
        inverse = root * root
        factor = [c * inverse for c in columns[k]]
        factor[0] = jnp.where(place > at, factor[0], 0.0)
        for j in range(k + 1, size):
            pivot = row_of(columns[k][j // SUB - own], j % SUB)
            shift = j // SUB - own
            columns[j] = [c - factor[i + shift] * pivot for i, c in enumerate(columns[j])]
        for h in range(width // LANES):
            pivot = row_of(rows[own][h], at)
            for i in range(own if at < SUB - 1 else own + 1, tiles):
                rows[i][h] = rows[i][h] - factor[i - own] * pivot
    return jnp.concatenate(
        [jnp.concatenate([part * scales[i] for part in rows[i]], axis=1) for i in range(tiles)], axis=0
    )


def iterate(gram_high, gram_low, basis, count):
    def turn(t):
        now = basis[...]
        high, low = halves(now)
        dot = functools.partial(jnp.dot, preferred_element_type=jnp.float32)
        moved = dot(high, gram_high[...]) + dot(low, gram_high[...]) + dot(high, gram_low[...])
        basis[...] = jnp.where(t < count, orthonormal_rows(moved), now)

    pl.loop(0, ITERS)(turn)


def subspace_kernel(rows, frames, count, rank, valid, gram, start, out, high, low, basis):
    high[...] = jnp.zeros_like(high)
    low[...] = jnp.zeros_like(low)
    basis[...] = jnp.zeros_like(basis)
    g_high, g_low = halves(gram[...] * (1.0 / rows))
    high[:frames, :frames] = g_high
    low[:frames, :frames] = g_low
    basis[:, :frames] = start[...]
    iterate(high, low, basis, count[0])
    kept = lax.broadcasted_iota(jnp.int32, basis.shape, 0) < jnp.where(valid[0] > 0, rank[0], 0)
    out[...] = jnp.where(kept, basis[...], 0.0).astype(out.dtype)


def truncated_basis(gram, start, count, rank, valid, rows):
    frames, size = start.shape
    wide = padded(frames)
    smem = pl.BlockSpec(memory_space=pltpu.SMEM)
    vmem = pl.BlockSpec(memory_space=pltpu.VMEM)
    return pl.pallas_call(
        functools.partial(subspace_kernel, rows, frames),
        out_shape=jax.ShapeDtypeStruct((size, wide), jnp.bfloat16),
        in_specs=[smem, smem, smem, vmem, vmem],
        out_specs=vmem,
        scratch_shapes=[
            pltpu.VMEM((wide, wide), jnp.bfloat16),
            pltpu.VMEM((wide, wide), jnp.bfloat16),
            pltpu.VMEM((size, wide), jnp.float32),
        ],
        name="subspace",
    )(count, rank, valid, gram, start.T)


def clutter_kernel(
    rows, chunks, echoes_hbm, start_hbm, rank_hbm, count_hbm, out, echoes,
    gram, sent, got, high, low, basis, mine, other, start, rank, count, load, sems,
):
    row, col = lax.axis_index("gx"), lax.axis_index("gy")
    cols = lax.axis_size("gy")
    size, frames = start.shape
    wide = gram.shape[1]
    part = echoes.shape[0] // chunks
    slab = lambda i: pl.ds(i * part, part)
    loads = [
        pltpu.make_async_copy(echoes_hbm.at[slab(i)], echoes.at[slab(i)], load.at[3 + i]) for i in range(chunks)
    ]
    small = [
        pltpu.make_async_copy(start_hbm, start, load.at[2]),
    ]
    partner = (1 - row, col)
    side = 1 - 2 * row
    far = (1 - row, col + side)
    exists = jnp.where(row == 0, col + 1 < cols, col >= 1)
    barrier = pltpu.get_barrier_semaphore()
    pl.semaphore_signal(barrier, inc=1, device_id=partner, device_id_type=MESH)

    @pl.when(exists)
    def _():
        pl.semaphore_signal(barrier, inc=1, device_id=far, device_id_type=MESH)

    for copy in loads + small:
        copy.start()

    def swap(source, target, at, peer):
        return pltpu.make_async_remote_copy(
            src_ref=source,
            dst_ref=target,
            send_sem=sems.at[2 * at],
            recv_sem=sems.at[2 * at + 1],
            device_id=peer,
            device_id_type=MESH,
        )

    high[...] = jnp.zeros_like(high)
    low[...] = jnp.zeros_like(low)
    basis[...] = jnp.zeros_like(basis)
    gram[...] = jnp.zeros_like(gram)
    total = None
    for i in range(chunks):
        loads[i].wait()
        block = echoes[i * part : (i + 1) * part, :]
        term = lax.dot_general(block, block, (((0,), (0,)), ((), ())), preferred_element_type=jnp.float32)
        total = term if total is None else total + term
    for copy in small:
        copy.wait()
    basis[:, :frames] = start[...]
    gram[:, :frames] = total
    sent[0] = gram[...].astype(jnp.bfloat16)

    @pl.when(exists)
    def _():
        pl.semaphore_wait(barrier, 2)

    @pl.when(jnp.logical_not(exists))
    def _():
        pl.semaphore_wait(barrier, 1)

    chip = swap(sent.at[0], got.at[0], 0, partner)
    chip.start()
    chip.wait()
    gram[...] = gram[...] + got[0].astype(jnp.float32)
    lane = lax.broadcasted_iota(jnp.int32, gram.shape, 1)
    rank_here = rank_hbm[0, 0, 0].astype(jnp.float32)
    count_here = count_hbm[0, 0, 0].astype(jnp.float32)
    sent[1] = jnp.where(
        lane == frames, rank_here, jnp.where(lane == frames + 1, count_here, gram[...])
    ).astype(jnp.bfloat16)

    @pl.when(exists)
    def _():
        top = swap(sent.at[1, :LANES, :LANES], got.at[1, :LANES, :LANES], 1, far)
        bottom = swap(sent.at[1, LANES:], got.at[1, LANES:], 3, far)
        top.start()
        bottom.start()
        top.wait()
        bottom.wait()

    @pl.when(jnp.logical_not(exists))
    def _():
        got[1] = jnp.zeros_like(got[1])

    picks = got[1, LANES:, LANES:].astype(jnp.float32)[:SUB, :]
    pick = lambda at, here: jnp.where(
        row == 0, here, jnp.broadcast_to(picks[0:1, frames - LANES + at : frames - LANES + at + 1], basis.shape)
    )
    rank_mine, count_mine = pick(0, rank_here), pick(1, count_here)
    total = jnp.where(lane < frames, gram[...] + got[1].astype(jnp.float32), 0.0) * (1.0 / rows)
    below = jnp.concatenate([total[LANES:, :LANES], jnp.zeros((wide - frames, LANES), jnp.float32)], axis=0)
    pieces = (
        (slice(0, LANES), slice(0, LANES), total[:LANES, :LANES]),
        (slice(LANES, frames), slice(0, wide), total[LANES:, :]),
        (slice(0, LANES), slice(LANES, wide), below.T),
    )
    for at, lanes, piece in pieces:
        g_high, g_low = halves(piece)
        high[at, lanes] = g_high
        low[at, lanes] = g_low
    iterate(high, low, basis, count_mine)
    index = lax.broadcasted_iota(jnp.int32, basis.shape, 0).astype(jnp.float32)
    kept = index < jnp.where(exists, rank_mine, 0.0)
    mine[...] = jnp.where(kept, basis[...], 0.0).astype(mine.dtype)
    pair = swap(mine, other, 2, partner)
    pair.start()
    pair.wait()
    own, theirs = mine[...], other[...]
    out[:size, :] = jnp.where(row == 0, own, theirs)
    out[size:, :] = jnp.where(row == 0, theirs, own)


def clutter_bases(echoes, start, rank, count, voxels):
    frames, size = start.shape
    wide = padded(frames + 2)
    chunks = 8
    hbm = pl.BlockSpec(memory_space=pltpu.HBM)
    vmem = pl.BlockSpec(memory_space=pltpu.VMEM)
    square = pltpu.VMEM((wide, wide), jnp.bfloat16)
    return pl.pallas_call(
        functools.partial(clutter_kernel, voxels, chunks),
        out_shape=[
            jax.ShapeDtypeStruct((2 * size, wide), jnp.bfloat16),
            jax.ShapeDtypeStruct(echoes.shape, echoes.dtype),
        ],
        in_specs=[hbm] * 2 + [pl.BlockSpec(memory_space=pltpu.SMEM)] * 2,
        out_specs=[vmem] * 2,
        scratch_shapes=[
            pltpu.VMEM((frames, wide), jnp.float32),
            pltpu.VMEM((2, frames, wide), jnp.bfloat16),
            pltpu.VMEM((2, frames, wide), jnp.bfloat16),
            square,
            square,
            pltpu.VMEM((size, wide), jnp.float32),
            pltpu.VMEM((size, wide), jnp.bfloat16),
            pltpu.VMEM((size, wide), jnp.bfloat16),
            pltpu.VMEM((size, frames), jnp.float32),
            pltpu.SMEM(rank.shape, jnp.int32),
            pltpu.SMEM(count.shape, jnp.int32),
            pltpu.SemaphoreType.DMA((3 + chunks,)),
            pltpu.SemaphoreType.DMA((8,)),
        ],
        compiler_params=pltpu.CompilerParams(collective_id=0, has_side_effects=True, vmem_limit_bytes=GRANT),
        name="clutter",
    )(*(pltpu.with_memory_space_constraint(x, pltpu.HBM) for x in (echoes, start.T)), rank, count)


def project_kernel(span, frames, echoes, vectors, scale_y, scale_x, out):
    base = pl.program_id(0) * (echoes.shape[0] // scale_y.shape[0])
    chunk = scale_y.shape[0]
    q = vectors[:, :frames]
    for part in range(echoes.shape[0] // chunk):
        at = pl.ds(part * chunk, chunk)
        local = echoes[at, :]
        coeff = nt(local, q) * (scale_y[...] * scale_x[pl.ds(base + part, 1), :])
        clutter = jnp.dot(coeff.astype(jnp.bfloat16), q, preferred_element_type=jnp.float32)
        out[at, :] = (local.astype(jnp.float32) - clutter).astype(out.dtype)


def project(echoes, vectors, scale_y, scale_x):
    voxels, frames = echoes.shape
    span = scale_x.shape[0]
    steps = 4
    while span % steps:
        steps //= 2
    whole = lambda a: pl.BlockSpec(a.shape, lambda i: (0, 0))
    return pl.pallas_call(
        functools.partial(project_kernel, span, frames),
        out_shape=jax.ShapeDtypeStruct(echoes.shape, echoes.dtype),
        grid=(steps,),
        in_specs=[
            pl.BlockSpec((voxels // steps, frames), lambda i: (i, 0)),
            whole(vectors),
            whole(scale_y),
            whole(scale_x),
        ],
        out_specs=pl.BlockSpec((voxels // steps, frames), lambda i: (i, 0)),
        name="project",
    )(echoes, vectors, scale_y, scale_x)


def separate_kernel(groups, echoes, vectors, out, result, base, slope, stores):
    span, lines, depth, frames = echoes.shape
    size = vectors.shape[0] // 2
    col, cols = lax.axis_index("gy"), lax.axis_size("gy")
    part = lines // groups
    line = lambda i: pl.ds(i * part, part)
    writes = [pltpu.make_async_copy(result.at[:, line(i)], out.at[:, line(i)], stores.at[i]) for i in range(groups)]
    projector = lambda q: lax.dot_general(q, q, (((0,), (0,)), ((), ())), preferred_element_type=jnp.float32)
    after = projector(vectors[:size, :frames])
    before = projector(vectors[size:, :frames])
    base[...] = before
    slope[...] = after - before
    for i in range(groups):
        for y in range(i * part, i * part + part):
            share = (1.0 + y) / (1.0 + lines)
            share = jnp.where(col == 0, 1.0, jnp.where(col == cols - 1, 0.0, share))
            mixed = (base[...] + share * slope[...]).astype(jnp.bfloat16)
            block = echoes[:, y].reshape(span * depth, frames)
            clutter = jnp.dot(block, mixed, preferred_element_type=jnp.float32)
            rest = (block.astype(jnp.float32) - clutter).astype(out.dtype)
            result[:, y] = rest.reshape(span, depth, frames)
        writes[i].start()
    for copy in writes:
        copy.wait()


def separate(echoes, vectors):
    groups = 4
    frames = echoes.shape[-1]
    anywhere = pl.BlockSpec(memory_space=pl.ANY)
    square = pltpu.VMEM((frames, frames), jnp.float32)
    return pl.pallas_call(
        functools.partial(separate_kernel, groups),
        out_shape=jax.ShapeDtypeStruct(echoes.shape, echoes.dtype),
        in_specs=[pl.BlockSpec(memory_space=pltpu.VMEM)] * 2,
        out_specs=anywhere,
        scratch_shapes=[
            pltpu.VMEM(echoes.shape, echoes.dtype),
            square,
            square,
            pltpu.SemaphoreType.DMA((groups,)),
        ],
        compiler_params=pltpu.CompilerParams(vmem_limit_bytes=GRANT),
        name="separate",
    )(echoes, vectors)


def shares(span, index, count):
    offset = jnp.arange(span, dtype=jnp.float32)
    here = tent(offset, 2.0 * span) * (index <= count - 2).astype(jnp.float32)
    before = tent(offset + span, 2.0 * span) * (index >= 1).astype(jnp.float32)
    return here / (here + before), before / (here + before)


def body(echoes, start, ranks, counts):
    span, _, depth, frames = echoes.shape
    size = start.shape[1]
    row, col = lax.axis_index("gx"), lax.axis_index("gy")
    rows, cols = lax.axis_size("gx"), lax.axis_size("gy")
    flat = echoes.reshape(-1, frames)
    voxels = 4 * flat.shape[0]

    def sent(x, axis, route):
        return lax.ppermute(x, axis, route)

    def basis(total, count, rank, valid):
        return truncated_basis(
            total, start, count.reshape(1), rank.reshape(1), valid.astype(jnp.int32).reshape(1), float(voxels)
        )

    if rows == 2:
        vectors, held = clutter_bases(flat, start, ranks, counts, float(voxels))
        return separate(held.reshape(echoes.shape), vectors)
    back = lambda n: [(i, i - 1) for i in range(1, n)]
    ahead = lambda n: [(i - 1, i) for i in range(1, n)]
    gram = lax.dot_general(flat, flat, (((0,), (0,)), ((), ())), preferred_element_type=jnp.float32)
    pair = gram + sent(gram.astype(jnp.bfloat16), "gy", back(cols)).astype(jnp.float32)
    total = pair + sent(pair.astype(jnp.bfloat16), "gx", back(rows)).astype(jnp.float32)
    own = basis(total, counts[0, 0, 0], ranks[0, 0, 0], (row <= rows - 2) & (col <= cols - 2))
    left = sent(own, "gy", ahead(cols))
    paired = jnp.concatenate([own, left])
    vectors = jnp.concatenate([paired, sent(paired, "gx", ahead(rows))])
    y_here, y_before = shares(span, col, cols)
    x_here, x_before = shares(span, row, rows)
    scale_ys = [y_here, y_before, y_here, y_before]
    scale_xs = [x_here, x_here, x_before, x_before]
    wide = lambda parts: jnp.concatenate([jnp.broadcast_to(p[:, None], (span, size)) for p in parts], axis=1)
    scale_y = jnp.repeat(wide(scale_ys), depth, axis=0)
    return project(flat, vectors, scale_y, wide(scale_xs)).reshape(echoes.shape)


def solution(mesh):
    placed = (P("gx", "gy", None, None), P(), P("gx", "gy", None), P("gx", "gy", None))
    return jax.shard_map(
        body, mesh=mesh, in_specs=placed, out_specs=P("gx", "gy", None, None), check_vma=False
    )
```

```python
import functools

import jax
import jax.numpy as jnp
from jax import lax
from jax.experimental import pallas as pl
from jax.experimental.pallas import tpu as pltpu
from jax.sharding import PartitionSpec as P

BZ = 16
ITERS = 4
LANES = 128
SUB = 8
BLOCK = 16
GRANT = 16 << 20
MESH = pl.DeviceIdType.MESH


def tent(offset, span):
    inside = (offset >= 0.0) & (offset < span)
    return jnp.where(inside, 1.0 + jnp.minimum(offset, span - 1.0 - offset), 0.0)


def padded(size):
    return -(-size // LANES) * LANES


def row_of(tile, k):
    return jnp.broadcast_to(tile[k : k + 1, :], tile.shape)


def halves(x):
    high = x.astype(jnp.bfloat16)
    return high, (x - high.astype(jnp.float32)).astype(jnp.bfloat16)


def nt(a, b):
    return lax.dot_general(a, b, (((1,), (1,)), ((), ())), preferred_element_type=jnp.float32)


def product(high, low, other_high, other_low, dot):
    size = high.shape[0]
    both = dot(jnp.concatenate([high, low], axis=0), other_high)
    return both[:size] + both[size:] + dot(high, other_low)


def orthonormal_rows(inner, moved, spare):
    size = inner.shape[0]
    tiles, lanes = size // SUB, moved.shape[1] // LANES
    rows = [
        [moved[SUB * i : SUB * i + SUB, LANES * h : LANES * h + LANES] for h in range(lanes)] for i in range(tiles)
    ]
    place = lax.broadcasted_iota(jnp.int32, (SUB, LANES), 0)
    scales = [None] * tiles
    spread = lambda x: jnp.broadcast_to(x, (SUB, LANES))
    for k in range(size):
        own, at = k // SUB, k % SUB
        if k % BLOCK == 0:
            end = min(k + BLOCK, size)
            if k == 0:
                source, base = [inner[SUB * i : SUB * i + SUB] for i in range(tiles)], 0
            else:
                source, base = [r[spare // LANES] for r in rows], spare % LANES
            columns = {
                j: {i: spread(source[i][:, base + j : base + j + 1]) for i in range(j // SUB, tiles)}
                for j in range(k, end)
            }
            pivot = row_of(columns[k][own], at)
        root = lax.rsqrt(pivot)
        scales[own] = root if at == 0 else jnp.where(place == at, root, scales[own])
        if k == size - 1:
            break
        inverse = root * root
        lines = {j: row_of(columns[k][j // SUB], j % SUB) for j in range(k + 1, end)}
        if k + 1 < end:
            pivot = row_of(columns[k + 1][(k + 1) // SUB], (k + 1) % SUB) - lines[k + 1] * lines[k + 1] * inverse
        factor = {i: c * inverse for i, c in columns[k].items()}
        factor[own] = jnp.where(place > at, factor[own], 0.0)
        for j in range(k + 1, end):
            columns[j] = {i: c - factor[i] * lines[j] for i, c in columns[j].items()}
        for h in reversed(range(lanes)):
            line = row_of(rows[own][h], at)
            for i in range(own if at < SUB - 1 else own + 1, tiles):
                rows[i][h] = rows[i][h] - factor[i] * line
    return jnp.concatenate(
        [jnp.concatenate([part * scales[i] for part in rows[i]], axis=1) for i in range(tiles)], axis=0
    )


def iterate(gram_high, gram_low, moved, basis, count, frames):
    size, wide = basis.shape
    spare = -(-frames // 16) * 16
    own = slice(spare, spare + size)
    moved[...] = product(*halves(basis[...]), gram_high[...], gram_low[...], nt)

    def turn(t):
        now = moved[...]
        high, low = halves(now)
        gram_high[own, :] = high
        gram_low[own, :] = low
        inner = product(high, low, high, low, nt)
        ahead = product(high, low, gram_high[...], gram_low[...], nt)
        both = orthonormal_rows(inner, jnp.concatenate([now, ahead], axis=1), wide + spare)
        basis[...] = jnp.where(t < count, both[:, :wide], basis[...])
        lane = lax.broadcasted_iota(jnp.int32, now.shape, 1)
        moved[...] = jnp.where(lane < frames, both[:, wide:], 0.0)

    pl.loop(0, ITERS)(turn)


def subspace_kernel(rows, frames, count, rank, valid, gram, start, out, high, low, moved, basis):
    high[...] = jnp.zeros_like(high)
    low[...] = jnp.zeros_like(low)
    basis[...] = jnp.zeros_like(basis)
    g_high, g_low = halves(gram[...] * (1.0 / rows))
    high[:frames, :frames] = g_high
    low[:frames, :frames] = g_low
    basis[:, :frames] = start[...]
    iterate(high, low, moved, basis, count[0], frames)
    kept = lax.broadcasted_iota(jnp.int32, basis.shape, 0) < jnp.where(valid[0] > 0, rank[0], 0)
    out[...] = jnp.where(kept, basis[...], 0.0).astype(out.dtype)


def truncated_basis(gram, start, count, rank, valid, rows):
    frames, size = start.shape
    wide = padded(frames)
    smem = pl.BlockSpec(memory_space=pltpu.SMEM)
    vmem = pl.BlockSpec(memory_space=pltpu.VMEM)
    return pl.pallas_call(
        functools.partial(subspace_kernel, rows, frames),
        out_shape=jax.ShapeDtypeStruct((size, wide), jnp.bfloat16),
        in_specs=[smem, smem, smem, vmem, vmem],
        out_specs=vmem,
        scratch_shapes=[
            pltpu.VMEM((wide, wide), jnp.bfloat16),
            pltpu.VMEM((wide, wide), jnp.bfloat16),
            pltpu.VMEM((size, wide), jnp.float32),
            pltpu.VMEM((size, wide), jnp.float32),
        ],
        name="subspace",
    )(count, rank, valid, gram, start.T)


def folded(gram):
    half, rest = LANES // 2, gram.shape[0] - LANES
    corner = pltpu.roll(gram[:half, :LANES], half, 1)
    lane = lax.broadcasted_iota(jnp.int32, corner.shape, 1)
    return jnp.concatenate(
        [
            gram[half:LANES, :LANES],
            gram[LANES:, :LANES],
            jnp.where(lane < half, gram[LANES : LANES + half, LANES:], corner),
            gram[LANES + half :, LANES:],
        ],
        axis=0,
    )


def unfolded(packed, rest):
    half = LANES // 2
    lower, cross = packed[:half], packed[half : half + rest]
    square, strip = packed[half + rest : LANES + rest], packed[LANES + rest :]
    lane = lax.broadcasted_iota(jnp.int32, square.shape, 1)
    filled = lambda above, x, below: jnp.concatenate(
        [jnp.zeros((n, LANES), jnp.float32) if isinstance(n, int) else n for n in (above, x, below) if not isinstance(n, int) or n],
        axis=0,
    )
    upper = filled(half, lower, 0).T
    side = filled(half, strip, half - strip.shape[0]).T
    first = jnp.where(lane < half, pltpu.roll(square, half, 1), upper[:half])
    mixed = jnp.where(lane < half, square, jnp.where(lane < rest, side[:half], 0.0))
    tail = jnp.where(lax.broadcasted_iota(jnp.int32, strip.shape, 1) < rest, strip, 0.0)
    here, there = slice(0, LANES), slice(LANES, 2 * LANES)
    return (
        (slice(0, half), here, first),
        (slice(half, LANES), here, lower),
        (slice(LANES, LANES + rest), here, cross),
        (slice(0, LANES), there, filled(0, cross, LANES - rest).T),
        (slice(LANES, LANES + half), there, mixed),
        (slice(LANES + half, LANES + rest), there, tail),
    )


def clutter_kernel(
    rows, chunks, echoes_hbm, start_hbm, rank_hbm, count_hbm, out, echoes,
    gram, sent, got, high, low, moved, basis, mine, other, start, rank, count, load, sems,
):
    row, col = lax.axis_index("gx"), lax.axis_index("gy")
    cols = lax.axis_size("gy")
    size, frames = start.shape
    wide = gram.shape[1]
    part = echoes.shape[0] // chunks
    slab = lambda i: pl.ds(i * part, part)
    loads = [
        pltpu.make_async_copy(echoes_hbm.at[slab(i)], echoes.at[slab(i)], load.at[3 + i]) for i in range(chunks)
    ]
    small = [
        pltpu.make_async_copy(start_hbm, start, load.at[2]),
    ]
    partner = (1 - row, col)
    side = 1 - 2 * row
    far = (1 - row, col + side)
    exists = jnp.where(row == 0, col + 1 < cols, col >= 1)
    barrier = pltpu.get_barrier_semaphore()
    pl.semaphore_signal(barrier, inc=1, device_id=partner, device_id_type=MESH)

    @pl.when(exists)
    def _():
        pl.semaphore_signal(barrier, inc=1, device_id=far, device_id_type=MESH)

    for copy in loads + small:
        copy.start()

    def swap(source, target, at, peer):
        return pltpu.make_async_remote_copy(
            src_ref=source,
            dst_ref=target,
            send_sem=sems.at[2 * at],
            recv_sem=sems.at[2 * at + 1],
            device_id=peer,
            device_id_type=MESH,
        )

    high[...] = jnp.zeros_like(high)
    low[...] = jnp.zeros_like(low)
    basis[...] = jnp.zeros_like(basis)
    gram[...] = jnp.zeros_like(gram)
    total = None
    for i in range(chunks):
        loads[i].wait()
        block = echoes[i * part : (i + 1) * part, :]
        term = lax.dot_general(block, block, (((0,), (0,)), ((), ())), preferred_element_type=jnp.float32)
        total = term if total is None else total + term
    for copy in small:
        copy.wait()
    basis[:, :frames] = start[...]
    gram[:, :frames] = total
    mine_sum = folded(gram)
    sent[0] = mine_sum.astype(jnp.bfloat16)

    @pl.when(exists)
    def _():
        pl.semaphore_wait(barrier, 2)

    @pl.when(jnp.logical_not(exists))
    def _():
        pl.semaphore_wait(barrier, 1)

    chip = swap(sent.at[0], got.at[0], 0, partner)
    chip.start()
    chip.wait()
    chip_sum = mine_sum + got[0].astype(jnp.float32)
    rank_here = rank_hbm[0, 0, 0].astype(jnp.float32)
    count_here = count_hbm[0, 0, 0].astype(jnp.float32)
    rest = frames - LANES
    lane = lax.broadcasted_iota(jnp.int32, (SUB, LANES), 1)
    strip = jnp.where(lane == rest, rank_here, jnp.where(lane == rest + 1, count_here, chip_sum[-SUB:]))
    sent[1] = jnp.concatenate([chip_sum[:-SUB], strip], axis=0).astype(jnp.bfloat16)

    @pl.when(exists)
    def _():
        over = swap(sent.at[1], got.at[1], 1, far)
        over.start()
        over.wait()

    @pl.when(jnp.logical_not(exists))
    def _():
        got[1] = jnp.zeros_like(got[1])

    theirs = got[1].astype(jnp.float32)
    pick = lambda at, here: jnp.where(
        row == 0, here, jnp.broadcast_to(theirs[-SUB : -SUB + 1, rest + at : rest + at + 1], basis.shape)
    )
    rank_mine, count_mine = pick(0, rank_here), pick(1, count_here)
    for at, lanes, piece in unfolded((chip_sum + theirs) * (1.0 / rows), rest):
        g_high, g_low = halves(piece)
        high[at, lanes] = g_high
        low[at, lanes] = g_low
    iterate(high, low, moved, basis, count_mine, frames)
    index = lax.broadcasted_iota(jnp.int32, basis.shape, 0).astype(jnp.float32)
    kept = index < jnp.where(exists, rank_mine, 0.0)
    mine[...] = jnp.where(kept, basis[...], 0.0).astype(mine.dtype)
    pair = swap(mine, other, 2, partner)
    pair.start()
    pair.wait()
    own, theirs = mine[...], other[...]
    out[:size, :] = jnp.where(row == 0, own, theirs)
    out[size:, :] = jnp.where(row == 0, theirs, own)


def clutter_bases(echoes, start, rank, count, voxels):
    frames, size = start.shape
    wide = padded(frames + 2)
    chunks = 2
    hbm = pl.BlockSpec(memory_space=pltpu.HBM)
    vmem = pl.BlockSpec(memory_space=pltpu.VMEM)
    square = pltpu.VMEM((wide, wide), jnp.bfloat16)
    return pl.pallas_call(
        functools.partial(clutter_kernel, voxels, chunks),
        out_shape=[
            jax.ShapeDtypeStruct((2 * size, wide), jnp.bfloat16),
            jax.ShapeDtypeStruct(echoes.shape, echoes.dtype),
        ],
        in_specs=[hbm] * 2 + [pl.BlockSpec(memory_space=pltpu.SMEM)] * 2,
        out_specs=[vmem] * 2,
        scratch_shapes=[
            pltpu.VMEM((frames, wide), jnp.float32),
            pltpu.VMEM((2, 2 * frames - 3 * LANES // 2, LANES), jnp.bfloat16),
            pltpu.VMEM((2, 2 * frames - 3 * LANES // 2, LANES), jnp.bfloat16),
            square,
            square,
            pltpu.VMEM((size, wide), jnp.float32),
            pltpu.VMEM((size, wide), jnp.float32),
            pltpu.VMEM((size, wide), jnp.bfloat16),
            pltpu.VMEM((size, wide), jnp.bfloat16),
            pltpu.VMEM((size, frames), jnp.float32),
            pltpu.SMEM(rank.shape, jnp.int32),
            pltpu.SMEM(count.shape, jnp.int32),
            pltpu.SemaphoreType.DMA((3 + chunks,)),
            pltpu.SemaphoreType.DMA((8,)),
        ],
        compiler_params=pltpu.CompilerParams(collective_id=0, has_side_effects=True, vmem_limit_bytes=GRANT),
        name="clutter",
    )(*(pltpu.with_memory_space_constraint(x, pltpu.HBM) for x in (echoes, start.T)), rank, count)


def project_kernel(span, frames, echoes, vectors, scale_y, scale_x, out):
    base = pl.program_id(0) * (echoes.shape[0] // scale_y.shape[0])
    chunk = scale_y.shape[0]
    q = vectors[:, :frames]
    for part in range(echoes.shape[0] // chunk):
        at = pl.ds(part * chunk, chunk)
        local = echoes[at, :]
        coeff = nt(local, q) * (scale_y[...] * scale_x[pl.ds(base + part, 1), :])
        clutter = jnp.dot(coeff.astype(jnp.bfloat16), q, preferred_element_type=jnp.float32)
        out[at, :] = (local.astype(jnp.float32) - clutter).astype(out.dtype)


def project(echoes, vectors, scale_y, scale_x):
    voxels, frames = echoes.shape
    span = scale_x.shape[0]
    steps = 4
    while span % steps:
        steps //= 2
    whole = lambda a: pl.BlockSpec(a.shape, lambda i: (0, 0))
    return pl.pallas_call(
        functools.partial(project_kernel, span, frames),
        out_shape=jax.ShapeDtypeStruct(echoes.shape, echoes.dtype),
        grid=(steps,),
        in_specs=[
            pl.BlockSpec((voxels // steps, frames), lambda i: (i, 0)),
            whole(vectors),
            whole(scale_y),
            whole(scale_x),
        ],
        out_specs=pl.BlockSpec((voxels // steps, frames), lambda i: (i, 0)),
        name="project",
    )(echoes, vectors, scale_y, scale_x)


def separate_kernel(groups, echoes, vectors, out, result, base, slope, stores):
    span, lines, depth, frames = echoes.shape
    size = vectors.shape[0] // 2
    col, cols = lax.axis_index("gy"), lax.axis_size("gy")
    part = lines // groups
    line = lambda i: pl.ds(i * part, part)
    writes = [pltpu.make_async_copy(result.at[:, line(i)], out.at[:, line(i)], stores.at[i]) for i in range(groups)]
    projector = lambda q: lax.dot_general(q, q, (((0,), (0,)), ((), ())), preferred_element_type=jnp.float32)
    after = projector(vectors[:size, :frames])
    before = projector(vectors[size:, :frames])
    base[...] = before
    slope[...] = after - before
    for i in range(groups):
        for y in range(i * part, i * part + part):
            share = (1.0 + y) / (1.0 + lines)
            share = jnp.where(col == 0, 1.0, jnp.where(col == cols - 1, 0.0, share))
            mixed = (base[...] + share * slope[...]).astype(jnp.bfloat16)
            block = echoes[:, y].reshape(span * depth, frames)
            clutter = jnp.dot(block, mixed, preferred_element_type=jnp.float32)
            rest = (block.astype(jnp.float32) - clutter).astype(out.dtype)
            result[:, y] = rest.reshape(span, depth, frames)
        writes[i].start()
    for copy in writes:
        copy.wait()


def separate(echoes, vectors):
    groups = 4
    frames = echoes.shape[-1]
    anywhere = pl.BlockSpec(memory_space=pl.ANY)
    square = pltpu.VMEM((frames, frames), jnp.float32)
    return pl.pallas_call(
        functools.partial(separate_kernel, groups),
        out_shape=jax.ShapeDtypeStruct(echoes.shape, echoes.dtype),
        in_specs=[pl.BlockSpec(memory_space=pltpu.VMEM)] * 2,
        out_specs=anywhere,
        scratch_shapes=[
            pltpu.VMEM(echoes.shape, echoes.dtype),
            square,
            square,
            pltpu.SemaphoreType.DMA((groups,)),
        ],
        compiler_params=pltpu.CompilerParams(vmem_limit_bytes=GRANT),
        name="separate",
    )(echoes, vectors)


def shares(span, index, count):
    offset = jnp.arange(span, dtype=jnp.float32)
    here = tent(offset, 2.0 * span) * (index <= count - 2).astype(jnp.float32)
    before = tent(offset + span, 2.0 * span) * (index >= 1).astype(jnp.float32)
    return here / (here + before), before / (here + before)


def body(echoes, start, ranks, counts):
    span, _, depth, frames = echoes.shape
    size = start.shape[1]
    row, col = lax.axis_index("gx"), lax.axis_index("gy")
    rows, cols = lax.axis_size("gx"), lax.axis_size("gy")
    flat = echoes.reshape(-1, frames)
    voxels = 4 * flat.shape[0]

    def sent(x, axis, route):
        return lax.ppermute(x, axis, route)

    def basis(total, count, rank, valid):
        return truncated_basis(
            total, start, count.reshape(1), rank.reshape(1), valid.astype(jnp.int32).reshape(1), float(voxels)
        )

    if rows == 2:
        vectors, held = clutter_bases(flat, start, ranks, counts, float(voxels))
        return separate(held.reshape(echoes.shape), vectors)
    back = lambda n: [(i, i - 1) for i in range(1, n)]
    ahead = lambda n: [(i - 1, i) for i in range(1, n)]
    gram = lax.dot_general(flat, flat, (((0,), (0,)), ((), ())), preferred_element_type=jnp.float32)
    pair = gram + sent(gram.astype(jnp.bfloat16), "gy", back(cols)).astype(jnp.float32)
    total = pair + sent(pair.astype(jnp.bfloat16), "gx", back(rows)).astype(jnp.float32)
    own = basis(total, counts[0, 0, 0], ranks[0, 0, 0], (row <= rows - 2) & (col <= cols - 2))
    left = sent(own, "gy", ahead(cols))
    paired = jnp.concatenate([own, left])
    vectors = jnp.concatenate([paired, sent(paired, "gx", ahead(rows))])
    y_here, y_before = shares(span, col, cols)
    x_here, x_before = shares(span, row, rows)
    scale_ys = [y_here, y_before, y_here, y_before]
    scale_xs = [x_here, x_here, x_before, x_before]
    wide = lambda parts: jnp.concatenate([jnp.broadcast_to(p[:, None], (span, size)) for p in parts], axis=1)
    scale_y = jnp.repeat(wide(scale_ys), depth, axis=0)
    return project(flat, vectors, scale_y, wide(scale_xs)).reshape(echoes.shape)


def solution(mesh):
    placed = (P("gx", "gy", None, None), P(), P("gx", "gy", None), P("gx", "gy", None))
    return jax.shard_map(
        body, mesh=mesh, in_specs=placed, out_specs=P("gx", "gy", None, None), check_vma=False
    )
```

```python
import functools

import jax
import jax.numpy as jnp
from jax import lax
from jax.experimental import pallas as pl
from jax.experimental.pallas import tpu as pltpu
from jax.sharding import PartitionSpec as P

BZ = 16
ITERS = 4
LANES = 128
SUB = 8
BLOCK = 16
HEAD = 16
GRANT = 16 << 20
MESH = pl.DeviceIdType.MESH


def tent(offset, span):
    inside = (offset >= 0.0) & (offset < span)
    return jnp.where(inside, 1.0 + jnp.minimum(offset, span - 1.0 - offset), 0.0)


def padded(size):
    return -(-size // LANES) * LANES


def row_of(tile, k):
    return jnp.broadcast_to(tile[k : k + 1, :], tile.shape)


def halves(x):
    high = x.astype(jnp.bfloat16)
    return high, (x - high.astype(jnp.float32)).astype(jnp.bfloat16)


def nt(a, b):
    return lax.dot_general(a, b, (((1,), (1,)), ((), ())), preferred_element_type=jnp.float32)


def product(high, low, other_high, other_low, dot):
    size = high.shape[0]
    both = dot(jnp.concatenate([high, low], axis=0), other_high)
    return both[:size] + both[size:] + dot(high, other_low)


def orthonormal_rows(inner, moved, spare):
    size = inner.shape[0]
    tiles, lanes = size // SUB, moved.shape[1] // LANES
    rows = [
        [moved[SUB * i : SUB * i + SUB, LANES * h : LANES * h + LANES] for h in range(lanes)] for i in range(tiles)
    ]
    place = lax.broadcasted_iota(jnp.int32, (SUB, LANES), 0)
    scales = [None] * tiles
    spread = lambda x: jnp.broadcast_to(x, (SUB, LANES))
    for k in range(size):
        own, at = k // SUB, k % SUB
        if k % BLOCK == 0:
            end = min(k + BLOCK, size)
            if k == 0:
                source, base = [inner[SUB * i : SUB * i + SUB] for i in range(tiles)], 0
            else:
                source, base = [r[spare // LANES] for r in rows], spare % LANES
            columns = {
                j: {i: spread(source[i][:, base + j : base + j + 1]) for i in range(j // SUB, tiles)}
                for j in range(k, end)
            }
            pivot = row_of(columns[k][own], at)
        root = lax.rsqrt(pivot)
        scales[own] = root if at == 0 else jnp.where(place == at, root, scales[own])
        if k == size - 1:
            break
        inverse = root * root
        lines = {j: row_of(columns[k][j // SUB], j % SUB) for j in range(k + 1, end)}
        if k + 1 < end:
            pivot = row_of(columns[k + 1][(k + 1) // SUB], (k + 1) % SUB) - lines[k + 1] * lines[k + 1] * inverse
        factor = {i: c * inverse for i, c in columns[k].items()}
        factor[own] = jnp.where(place > at, factor[own], 0.0)
        for j in range(k + 1, end):
            columns[j] = {i: c - factor[i] * lines[j] for i, c in columns[j].items()}
        for h in reversed(range(lanes)):
            line = row_of(rows[own][h], at)
            for i in range(own if at < SUB - 1 else own + 1, tiles):
                rows[i][h] = rows[i][h] - factor[i] * line
    return jnp.concatenate(
        [jnp.concatenate([part * scales[i] for part in rows[i]], axis=1) for i in range(tiles)], axis=0
    )


def iterate(gram_high, gram_low, moved, basis, count, frames):
    size, wide = basis.shape
    spare = -(-frames // 16) * 16
    own = slice(spare, spare + size)
    moved[...] = product(*halves(basis[...]), gram_high[...], gram_low[...], nt)

    def turn(t):
        now = moved[...]
        high, low = halves(now)
        gram_high[own, :] = high
        gram_low[own, :] = low
        inner = product(high, low, high, low, nt)
        ahead = product(high, low, gram_high[...], gram_low[...], nt)
        both = orthonormal_rows(inner, jnp.concatenate([now, ahead], axis=1), wide + spare)
        basis[...] = jnp.where(t < count, both[:, :wide], basis[...])
        lane = lax.broadcasted_iota(jnp.int32, now.shape, 1)
        moved[...] = jnp.where(lane < frames, both[:, wide:], 0.0)

    pl.loop(0, ITERS)(turn)


def subspace_kernel(rows, frames, count, rank, valid, gram, start, out, high, low, moved, basis):
    high[...] = jnp.zeros_like(high)
    low[...] = jnp.zeros_like(low)
    basis[...] = jnp.zeros_like(basis)
    g_high, g_low = halves(gram[...] * (1.0 / rows))
    high[:frames, :frames] = g_high
    low[:frames, :frames] = g_low
    basis[:, :frames] = start[...]
    iterate(high, low, moved, basis, count[0], frames)
    kept = lax.broadcasted_iota(jnp.int32, basis.shape, 0) < jnp.where(valid[0] > 0, rank[0], 0)
    out[...] = jnp.where(kept, basis[...], 0.0).astype(out.dtype)


def truncated_basis(gram, start, count, rank, valid, rows):
    frames, size = start.shape
    wide = padded(frames)
    smem = pl.BlockSpec(memory_space=pltpu.SMEM)
    vmem = pl.BlockSpec(memory_space=pltpu.VMEM)
    return pl.pallas_call(
        functools.partial(subspace_kernel, rows, frames),
        out_shape=jax.ShapeDtypeStruct((size, wide), jnp.bfloat16),
        in_specs=[smem, smem, smem, vmem, vmem],
        out_specs=vmem,
        scratch_shapes=[
            pltpu.VMEM((wide, wide), jnp.bfloat16),
            pltpu.VMEM((wide, wide), jnp.bfloat16),
            pltpu.VMEM((size, wide), jnp.float32),
            pltpu.VMEM((size, wide), jnp.float32),
        ],
        name="subspace",
    )(count, rank, valid, gram, start.T)


def folded(gram):
    half, rest = LANES // 2, gram.shape[0] - LANES
    corner = pltpu.roll(gram[:half, :LANES], half, 1)
    lane = lax.broadcasted_iota(jnp.int32, corner.shape, 1)
    return jnp.concatenate(
        [
            gram[half:LANES, :LANES],
            gram[LANES:, :LANES],
            jnp.where(lane < half, gram[LANES : LANES + half, LANES:], corner),
            gram[LANES + half :, LANES:],
        ],
        axis=0,
    )


def unfolded(packed, rest):
    half = LANES // 2
    lower, cross = packed[:half], packed[half : half + rest]
    square, strip = packed[half + rest : LANES + rest], packed[LANES + rest :]
    lane = lax.broadcasted_iota(jnp.int32, square.shape, 1)
    filled = lambda above, x, below: jnp.concatenate(
        [jnp.zeros((n, LANES), jnp.float32) if isinstance(n, int) else n for n in (above, x, below) if not isinstance(n, int) or n],
        axis=0,
    )
    upper = filled(half, lower, 0).T
    side = filled(half, strip, half - strip.shape[0]).T
    first = jnp.where(lane < half, pltpu.roll(square, half, 1), upper[:half])
    mixed = jnp.where(lane < half, square, jnp.where(lane < rest, side[:half], 0.0))
    tail = jnp.where(lax.broadcasted_iota(jnp.int32, strip.shape, 1) < rest, strip, 0.0)
    here, there = slice(0, LANES), slice(LANES, 2 * LANES)
    return (
        (slice(0, half), here, first),
        (slice(half, LANES), here, lower),
        (slice(LANES, LANES + rest), here, cross),
        (slice(0, LANES), there, filled(0, cross, LANES - rest).T),
        (slice(LANES, LANES + half), there, mixed),
        (slice(LANES + half, LANES + rest), there, tail),
    )


def clutter_kernel(
    rows, chunks, echoes_hbm, start_hbm, rank_hbm, count_hbm, out, echoes,
    gram, sent, got, early, high, low, moved, basis, mine, other, start, rank, count, load, sems,
):
    row, col = lax.axis_index("gx"), lax.axis_index("gy")
    cols = lax.axis_size("gy")
    size, frames = start.shape
    wide = gram.shape[1]
    part = echoes.shape[0] // chunks
    slab = lambda i: pl.ds(i * part, part)
    loads = [
        pltpu.make_async_copy(echoes_hbm.at[slab(i)], echoes.at[slab(i)], load.at[3 + i]) for i in range(chunks)
    ]
    small = [
        pltpu.make_async_copy(start_hbm, start, load.at[2]),
    ]
    partner = (1 - row, col)
    side = 1 - 2 * row
    far = (1 - row, col + side)
    before, after = col >= 1, col + 1 < cols
    exists = jnp.where(row == 0, after, before)
    down, up = (0, col - 1), (1, col + 1)
    barrier = pltpu.get_barrier_semaphore()
    meet = lambda peer: pl.semaphore_signal(barrier, inc=1, device_id=peer, device_id_type=MESH)
    meet(partner)

    @pl.when(before)
    def _():
        meet(down)

    @pl.when(after)
    def _():
        meet(up)

    @pl.when(exists)
    def _():
        meet((row, col + side))

    for copy in loads + small:
        copy.start()

    def swap(source, target, at, peer):
        return pltpu.make_async_remote_copy(
            src_ref=source,
            dst_ref=target,
            send_sem=sems.at[2 * at],
            recv_sem=sems.at[2 * at + 1],
            device_id=peer,
            device_id_type=MESH,
        )

    high[...] = jnp.zeros_like(high)
    low[...] = jnp.zeros_like(low)
    basis[...] = jnp.zeros_like(basis)
    gram[...] = jnp.zeros_like(gram)
    total = None
    for i in range(chunks):
        loads[i].wait()
        block = echoes[i * part : (i + 1) * part, :]
        term = lax.dot_general(block, block, (((0,), (0,)), ((), ())), preferred_element_type=jnp.float32)
        total = term if total is None else total + term
    for copy in small:
        copy.wait()
    basis[:, :frames] = start[...]
    gram[:, :frames] = total
    mine_sum = folded(gram)
    sent[0] = mine_sum.astype(jnp.bfloat16)

    pl.semaphore_wait(barrier, 1 + jnp.where(before, 1 + row, 0) + jnp.where(after, 2 - row, 0))
    chip = swap(sent.at[0], got.at[0], 0, partner)
    chip.start()
    head = early.shape[1]

    def hand(at, peer):
        return pltpu.make_async_remote_copy(
            src_ref=sent.at[0, :head],
            dst_ref=early.at[row],
            send_sem=sems.at[6 + at],
            recv_sem=sems.at[8 + row],
            device_id=peer,
            device_id_type=MESH,
        )

    @pl.when(before)
    def _():
        hand(0, down).start()

    @pl.when(after)
    def _():
        hand(1, up).start()

    chip.wait()
    chip_sum = mine_sum + got[0].astype(jnp.float32)
    rank_here = rank_hbm[0, 0, 0].astype(jnp.float32)
    count_here = count_hbm[0, 0, 0].astype(jnp.float32)
    rest = frames - LANES
    lane = lax.broadcasted_iota(jnp.int32, (SUB, LANES), 1)
    strip = jnp.where(lane == rest, rank_here, jnp.where(lane == rest + 1, count_here, chip_sum[-SUB:]))
    sent[1] = jnp.concatenate([chip_sum[:-SUB], strip], axis=0).astype(jnp.bfloat16)

    @pl.when(exists)
    def _():
        over = swap(sent.at[1, head:], got.at[1, head:], 1, far)
        over.start()
        for at in range(2):
            pltpu.make_async_remote_copy(
                src_ref=sent.at[0, :head],
                dst_ref=early.at[at],
                send_sem=sems.at[6],
                recv_sem=sems.at[8 + at],
                device_id=far,
                device_id_type=MESH,
            ).wait_recv()
        over.wait()

    @pl.when(jnp.logical_not(exists))
    def _():
        got[1, head:] = jnp.zeros_like(got[1, head:])
        early[...] = jnp.zeros_like(early)

    theirs = jnp.concatenate(
        [early[0].astype(jnp.float32) + early[1].astype(jnp.float32), got[1, head:].astype(jnp.float32)], axis=0
    )
    pick = lambda at, here: jnp.where(
        row == 0, here, jnp.broadcast_to(theirs[-SUB : -SUB + 1, rest + at : rest + at + 1], basis.shape)
    )
    rank_mine, count_mine = pick(0, rank_here), pick(1, count_here)
    for at, lanes, piece in unfolded((chip_sum + theirs) * (1.0 / rows), rest):
        g_high, g_low = halves(piece)
        high[at, lanes] = g_high
        low[at, lanes] = g_low
    iterate(high, low, moved, basis, count_mine, frames)
    index = lax.broadcasted_iota(jnp.int32, basis.shape, 0).astype(jnp.float32)
    kept = index < jnp.where(exists, rank_mine, 0.0)
    mine[...] = jnp.where(kept, basis[...], 0.0).astype(mine.dtype)
    pair = swap(mine, other, 2, partner)
    pair.start()

    @pl.when(before)
    def _():
        hand(0, down).wait_send()

    @pl.when(after)
    def _():
        hand(1, up).wait_send()

    pair.wait()
    own, theirs = mine[...], other[...]
    out[:size, :] = jnp.where(row == 0, own, theirs)
    out[size:, :] = jnp.where(row == 0, theirs, own)


def clutter_bases(echoes, start, rank, count, voxels):
    frames, size = start.shape
    wide = padded(frames + 2)
    chunks = 2
    hbm = pl.BlockSpec(memory_space=pltpu.HBM)
    vmem = pl.BlockSpec(memory_space=pltpu.VMEM)
    square = pltpu.VMEM((wide, wide), jnp.bfloat16)
    return pl.pallas_call(
        functools.partial(clutter_kernel, voxels, chunks),
        out_shape=[
            jax.ShapeDtypeStruct((2 * size, wide), jnp.bfloat16),
            jax.ShapeDtypeStruct(echoes.shape, echoes.dtype),
        ],
        in_specs=[hbm] * 2 + [pl.BlockSpec(memory_space=pltpu.SMEM)] * 2,
        out_specs=[vmem] * 2,
        scratch_shapes=[
            pltpu.VMEM((frames, wide), jnp.float32),
            pltpu.VMEM((2, 2 * frames - 3 * LANES // 2, LANES), jnp.bfloat16),
            pltpu.VMEM((2, 2 * frames - 3 * LANES // 2, LANES), jnp.bfloat16),
            pltpu.VMEM((2, (2 * frames - 3 * LANES // 2) // 32 * HEAD, LANES), jnp.bfloat16),
            square,
            square,
            pltpu.VMEM((size, wide), jnp.float32),
            pltpu.VMEM((size, wide), jnp.float32),
            pltpu.VMEM((size, wide), jnp.bfloat16),
            pltpu.VMEM((size, wide), jnp.bfloat16),
            pltpu.VMEM((size, frames), jnp.float32),
            pltpu.SMEM(rank.shape, jnp.int32),
            pltpu.SMEM(count.shape, jnp.int32),
            pltpu.SemaphoreType.DMA((3 + chunks,)),
            pltpu.SemaphoreType.DMA((10,)),
        ],
        compiler_params=pltpu.CompilerParams(collective_id=0, has_side_effects=True, vmem_limit_bytes=GRANT),
        name="clutter",
    )(*(pltpu.with_memory_space_constraint(x, pltpu.HBM) for x in (echoes, start.T)), rank, count)


def project_kernel(span, frames, echoes, vectors, scale_y, scale_x, out):
    base = pl.program_id(0) * (echoes.shape[0] // scale_y.shape[0])
    chunk = scale_y.shape[0]
    q = vectors[:, :frames]
    for part in range(echoes.shape[0] // chunk):
        at = pl.ds(part * chunk, chunk)
        local = echoes[at, :]
        coeff = nt(local, q) * (scale_y[...] * scale_x[pl.ds(base + part, 1), :])
        clutter = jnp.dot(coeff.astype(jnp.bfloat16), q, preferred_element_type=jnp.float32)
        out[at, :] = (local.astype(jnp.float32) - clutter).astype(out.dtype)


def project(echoes, vectors, scale_y, scale_x):
    voxels, frames = echoes.shape
    span = scale_x.shape[0]
    steps = 4
    while span % steps:
        steps //= 2
    whole = lambda a: pl.BlockSpec(a.shape, lambda i: (0, 0))
    return pl.pallas_call(
        functools.partial(project_kernel, span, frames),
        out_shape=jax.ShapeDtypeStruct(echoes.shape, echoes.dtype),
        grid=(steps,),
        in_specs=[
            pl.BlockSpec((voxels // steps, frames), lambda i: (i, 0)),
            whole(vectors),
            whole(scale_y),
            whole(scale_x),
        ],
        out_specs=pl.BlockSpec((voxels // steps, frames), lambda i: (i, 0)),
        name="project",
    )(echoes, vectors, scale_y, scale_x)


def separate_kernel(groups, echoes, vectors, out, result, base, slope, stores):
    span, lines, depth, frames = echoes.shape
    size = vectors.shape[0] // 2
    col, cols = lax.axis_index("gy"), lax.axis_size("gy")
    part = lines // groups
    line = lambda i: pl.ds(i * part, part)
    writes = [pltpu.make_async_copy(result.at[:, line(i)], out.at[:, line(i)], stores.at[i]) for i in range(groups)]
    projector = lambda q: lax.dot_general(q, q, (((0,), (0,)), ((), ())), preferred_element_type=jnp.float32)
    after = projector(vectors[:size, :frames])
    before = projector(vectors[size:, :frames])
    base[...] = before
    slope[...] = after - before
    for i in range(groups):
        for y in range(i * part, i * part + part):
            share = (1.0 + y) / (1.0 + lines)
            share = jnp.where(col == 0, 1.0, jnp.where(col == cols - 1, 0.0, share))
            mixed = (base[...] + share * slope[...]).astype(jnp.bfloat16)
            block = echoes[:, y].reshape(span * depth, frames)
            clutter = jnp.dot(block, mixed, preferred_element_type=jnp.float32)
            rest = (block.astype(jnp.float32) - clutter).astype(out.dtype)
            result[:, y] = rest.reshape(span, depth, frames)
        writes[i].start()
    for copy in writes:
        copy.wait()


def separate(echoes, vectors):
    groups = 8
    frames = echoes.shape[-1]
    anywhere = pl.BlockSpec(memory_space=pl.ANY)
    square = pltpu.VMEM((frames, frames), jnp.float32)
    return pl.pallas_call(
        functools.partial(separate_kernel, groups),
        out_shape=jax.ShapeDtypeStruct(echoes.shape, echoes.dtype),
        in_specs=[pl.BlockSpec(memory_space=pltpu.VMEM)] * 2,
        out_specs=anywhere,
        scratch_shapes=[
            pltpu.VMEM(echoes.shape, echoes.dtype),
            square,
            square,
            pltpu.SemaphoreType.DMA((groups,)),
        ],
        compiler_params=pltpu.CompilerParams(vmem_limit_bytes=GRANT),
        name="separate",
    )(echoes, vectors)


def shares(span, index, count):
    offset = jnp.arange(span, dtype=jnp.float32)
    here = tent(offset, 2.0 * span) * (index <= count - 2).astype(jnp.float32)
    before = tent(offset + span, 2.0 * span) * (index >= 1).astype(jnp.float32)
    return here / (here + before), before / (here + before)


def body(echoes, start, ranks, counts):
    span, _, depth, frames = echoes.shape
    size = start.shape[1]
    row, col = lax.axis_index("gx"), lax.axis_index("gy")
    rows, cols = lax.axis_size("gx"), lax.axis_size("gy")
    flat = echoes.reshape(-1, frames)
    voxels = 4 * flat.shape[0]

    def sent(x, axis, route):
        return lax.ppermute(x, axis, route)

    def basis(total, count, rank, valid):
        return truncated_basis(
            total, start, count.reshape(1), rank.reshape(1), valid.astype(jnp.int32).reshape(1), float(voxels)
        )

    if rows == 2:
        vectors, held = clutter_bases(flat, start, ranks, counts, float(voxels))
        return separate(held.reshape(echoes.shape), vectors)
    back = lambda n: [(i, i - 1) for i in range(1, n)]
    ahead = lambda n: [(i - 1, i) for i in range(1, n)]
    gram = lax.dot_general(flat, flat, (((0,), (0,)), ((), ())), preferred_element_type=jnp.float32)
    pair = gram + sent(gram.astype(jnp.bfloat16), "gy", back(cols)).astype(jnp.float32)
    total = pair + sent(pair.astype(jnp.bfloat16), "gx", back(rows)).astype(jnp.float32)
    own = basis(total, counts[0, 0, 0], ranks[0, 0, 0], (row <= rows - 2) & (col <= cols - 2))
    left = sent(own, "gy", ahead(cols))
    paired = jnp.concatenate([own, left])
    vectors = jnp.concatenate([paired, sent(paired, "gx", ahead(rows))])
    y_here, y_before = shares(span, col, cols)
    x_here, x_before = shares(span, row, rows)
    scale_ys = [y_here, y_before, y_here, y_before]
    scale_xs = [x_here, x_here, x_before, x_before]
    wide = lambda parts: jnp.concatenate([jnp.broadcast_to(p[:, None], (span, size)) for p in parts], axis=1)
    scale_y = jnp.repeat(wide(scale_ys), depth, axis=0)
    return project(flat, vectors, scale_y, wide(scale_xs)).reshape(echoes.shape)


def solution(mesh):
    placed = (P("gx", "gy", None, None), P(), P("gx", "gy", None), P("gx", "gy", None))
    return jax.shard_map(
        body, mesh=mesh, in_specs=placed, out_specs=P("gx", "gy", None, None), check_vma=False
    )
```

```python
import functools

import jax
import jax.numpy as jnp
from jax import lax
from jax.experimental import pallas as pl
from jax.experimental.pallas import tpu as pltpu
from jax.sharding import PartitionSpec as P

BZ = 16
ITERS = 4
LANES = 128
SUB = 8
BLOCK = 16
HEAD = 16
GRANT = 16 << 20
MESH = pl.DeviceIdType.MESH


def tent(offset, span):
    inside = (offset >= 0.0) & (offset < span)
    return jnp.where(inside, 1.0 + jnp.minimum(offset, span - 1.0 - offset), 0.0)


def padded(size):
    return -(-size // LANES) * LANES


def row_of(tile, k):
    return jnp.broadcast_to(tile[k : k + 1, :], tile.shape)


def halves(x):
    high = x.astype(jnp.bfloat16)
    return high, (x - high.astype(jnp.float32)).astype(jnp.bfloat16)


def nt(a, b):
    return lax.dot_general(a, b, (((1,), (1,)), ((), ())), preferred_element_type=jnp.float32)


def product(high, low, other_high, other_low, dot):
    size = high.shape[0]
    both = dot(jnp.concatenate([high, low], axis=0), other_high)
    return both[:size] + both[size:] + dot(high, other_low)


def orthonormal_rows(inner, moved, spare):
    size = inner.shape[0]
    tiles, lanes = size // SUB, moved.shape[1] // LANES
    rows = [
        [moved[SUB * i : SUB * i + SUB, LANES * h : LANES * h + LANES] for h in range(lanes)] for i in range(tiles)
    ]
    place = lax.broadcasted_iota(jnp.int32, (SUB, LANES), 0)
    scales = [None] * tiles
    spread = lambda x: jnp.broadcast_to(x, (SUB, LANES))
    for k in range(size):
        own, at = k // SUB, k % SUB
        if k % BLOCK == 0:
            end = min(k + BLOCK, size)
            if k == 0:
                source, base = [inner[SUB * i : SUB * i + SUB] for i in range(tiles)], 0
            else:
                source, base = [r[spare // LANES] for r in rows], spare % LANES
            columns = {
                j: {i: spread(source[i][:, base + j : base + j + 1]) for i in range(j // SUB, tiles)}
                for j in range(k, end)
            }
            columns[k] = {i: jnp.where(place >= 0, c, 0.0) for i, c in columns[k].items()}
            pivot = row_of(columns[k][own], at)
        root = lax.rsqrt(pivot)
        scales[own] = root if at == 0 else jnp.where(place == at, root, scales[own])
        if k == size - 1:
            break
        inverse = root * root
        lines = {j: row_of(columns[k][j // SUB], j % SUB) for j in range(k + 1, end)}
        if k + 1 < end:
            pivot = row_of(columns[k + 1][(k + 1) // SUB], (k + 1) % SUB) - lines[k + 1] * lines[k + 1] * inverse
        factor = {i: c * inverse for i, c in columns[k].items()}
        factor[own] = jnp.where(place > at, factor[own], 0.0)
        for j in range(k + 1, end):
            columns[j] = {i: c - factor[i] * lines[j] for i, c in columns[j].items()}
        for h in reversed(range(lanes)):
            line = row_of(rows[own][h], at)
            for i in range(own if at < SUB - 1 else own + 1, tiles):
                rows[i][h] = rows[i][h] - factor[i] * line
    return jnp.concatenate(
        [jnp.concatenate([part * scales[i] for part in rows[i]], axis=1) for i in range(tiles)], axis=0
    )


def iterate(gram_high, gram_low, basis, count, frames):
    size, wide = basis.shape
    spare = -(-frames // 16) * 16
    own = slice(spare, spare + size)
    basis[...] = product(*halves(basis[...]), gram_high[...], gram_low[...], nt)
    lane = lax.broadcasted_iota(jnp.int32, basis.shape, 1)

    def turn(t):
        now = basis[...]
        high, low = halves(now)
        gram_high[own, :] = high
        gram_low[own, :] = low
        inner = product(high, low, high, low, nt)
        ahead = product(high, low, gram_high[...], gram_low[...], nt)
        last = t == ITERS - 1
        rows = jnp.where((lane < frames) & last, now, ahead)
        done = orthonormal_rows(inner, rows, spare)
        basis[...] = jnp.where(lane < frames, jnp.where((t + 1 < count) | last, done, now), 0.0)

    pl.loop(0, ITERS)(turn)


def subspace_kernel(rows, frames, count, rank, valid, gram, start, out, high, low, basis):
    high[...] = jnp.zeros_like(high)
    low[...] = jnp.zeros_like(low)
    basis[...] = jnp.zeros_like(basis)
    g_high, g_low = halves(gram[...] * (1.0 / rows))
    high[:frames, :frames] = g_high
    low[:frames, :frames] = g_low
    basis[:, :frames] = start[...]
    iterate(high, low, basis, count[0], frames)
    kept = lax.broadcasted_iota(jnp.int32, basis.shape, 0) < jnp.where(valid[0] > 0, rank[0], 0)
    out[...] = jnp.where(kept, basis[...], 0.0).astype(out.dtype)


def truncated_basis(gram, start, count, rank, valid, rows):
    frames, size = start.shape
    wide = padded(frames)
    smem = pl.BlockSpec(memory_space=pltpu.SMEM)
    vmem = pl.BlockSpec(memory_space=pltpu.VMEM)
    return pl.pallas_call(
        functools.partial(subspace_kernel, rows, frames),
        out_shape=jax.ShapeDtypeStruct((size, wide), jnp.bfloat16),
        in_specs=[smem, smem, smem, vmem, vmem],
        out_specs=vmem,
        scratch_shapes=[
            pltpu.VMEM((wide, wide), jnp.bfloat16),
            pltpu.VMEM((wide, wide), jnp.bfloat16),
            pltpu.VMEM((size, wide), jnp.float32),
        ],
        name="subspace",
    )(count, rank, valid, gram, start.T)


def folded(gram):
    half, rest = LANES // 2, gram.shape[0] - LANES
    corner = pltpu.roll(gram[:half, :LANES], half, 1)
    lane = lax.broadcasted_iota(jnp.int32, corner.shape, 1)
    return jnp.concatenate(
        [
            gram[half:LANES, :LANES],
            gram[LANES:, :LANES],
            jnp.where(lane < half, gram[LANES : LANES + half, LANES:], corner),
            gram[LANES + half :, LANES:],
        ],
        axis=0,
    )


def unfolded(packed, rest):
    half = LANES // 2
    lower, cross = packed[:half], packed[half : half + rest]
    square, strip = packed[half + rest : LANES + rest], packed[LANES + rest :]
    lane = lax.broadcasted_iota(jnp.int32, square.shape, 1)
    filled = lambda above, x, below: jnp.concatenate(
        [jnp.zeros((n, LANES), jnp.float32) if isinstance(n, int) else n for n in (above, x, below) if not isinstance(n, int) or n],
        axis=0,
    )
    upper = filled(half, lower, 0).T
    side = filled(half, strip, half - strip.shape[0]).T
    first = jnp.where(lane < half, pltpu.roll(square, half, 1), upper[:half])
    mixed = jnp.where(lane < half, square, jnp.where(lane < rest, side[:half], 0.0))
    tail = jnp.where(lax.broadcasted_iota(jnp.int32, strip.shape, 1) < rest, strip, 0.0)
    here, there = slice(0, LANES), slice(LANES, 2 * LANES)
    return (
        (slice(0, half), here, first),
        (slice(half, LANES), here, lower),
        (slice(LANES, LANES + rest), here, cross),
        (slice(0, LANES), there, filled(0, cross, LANES - rest).T),
        (slice(LANES, LANES + half), there, mixed),
        (slice(LANES + half, LANES + rest), there, tail),
    )


def clutter_kernel(
    rows, chunks, echoes_hbm, start_hbm, rank_hbm, count_hbm, out, echoes,
    gram, sent, got, early, high, low, basis, mine, other, start, rank, count, load, sems,
):
    row, col = lax.axis_index("gx"), lax.axis_index("gy")
    cols = lax.axis_size("gy")
    size, frames = start.shape
    wide = gram.shape[1]
    part = echoes.shape[0] // chunks
    pieces = echoes.shape[0] // (load.shape[0] - 3)
    slab = lambda i: pl.ds(i * pieces, pieces)
    loads = [
        pltpu.make_async_copy(echoes_hbm.at[slab(i)], echoes.at[slab(i)], load.at[3 + i])
        for i in range(load.shape[0] - 3)
    ]
    small = [
        pltpu.make_async_copy(start_hbm, start, load.at[2]),
    ]
    partner = (1 - row, col)
    side = 1 - 2 * row
    far = (1 - row, col + side)
    before, after = col >= 1, col + 1 < cols
    exists = jnp.where(row == 0, after, before)
    down, up = (0, col - 1), (1, col + 1)
    barrier = pltpu.get_barrier_semaphore()
    meet = lambda peer: pl.semaphore_signal(barrier, inc=1, device_id=peer, device_id_type=MESH)
    meet(partner)

    @pl.when(before)
    def _():
        meet(down)

    @pl.when(after)
    def _():
        meet(up)

    @pl.when(exists)
    def _():
        meet((row, col + side))

    for copy in loads + small:
        copy.start()

    def swap(source, target, at, peer):
        return pltpu.make_async_remote_copy(
            src_ref=source,
            dst_ref=target,
            send_sem=sems.at[2 * at],
            recv_sem=sems.at[2 * at + 1],
            device_id=peer,
            device_id_type=MESH,
        )

    high[...] = jnp.zeros_like(high)
    low[...] = jnp.zeros_like(low)
    basis[...] = jnp.zeros_like(basis)
    gram[...] = jnp.zeros_like(gram)
    total = None
    for i in range(chunks):
        for copy in loads[i * len(loads) // chunks : (i + 1) * len(loads) // chunks]:
            copy.wait()
        block = echoes[i * part : (i + 1) * part, :]
        term = lax.dot_general(block, block, (((0,), (0,)), ((), ())), preferred_element_type=jnp.float32)
        total = term if total is None else total + term
    for copy in small:
        copy.wait()
    basis[:, :frames] = start[...]
    gram[:, :frames] = total
    mine_sum = folded(gram)
    sent[0] = mine_sum.astype(jnp.bfloat16)

    pl.semaphore_wait(barrier, 1 + jnp.where(before, 1 + row, 0) + jnp.where(after, 2 - row, 0))
    chip = swap(sent.at[0], got.at[0], 0, partner)
    chip.start()
    head = early.shape[1]

    def hand(at, peer):
        return pltpu.make_async_remote_copy(
            src_ref=sent.at[0, :head],
            dst_ref=early.at[row],
            send_sem=sems.at[6 + at],
            recv_sem=sems.at[8 + row],
            device_id=peer,
            device_id_type=MESH,
        )

    @pl.when(before)
    def _():
        hand(0, down).start()

    @pl.when(after)
    def _():
        hand(1, up).start()

    chip.wait()
    chip_sum = mine_sum + got[0].astype(jnp.float32)
    rank_here = rank_hbm[0, 0, 0].astype(jnp.float32)
    count_here = count_hbm[0, 0, 0].astype(jnp.float32)
    rest = frames - LANES
    lane = lax.broadcasted_iota(jnp.int32, (SUB, LANES), 1)
    strip = jnp.where(lane == rest, rank_here, jnp.where(lane == rest + 1, count_here, chip_sum[-SUB:]))
    sent[1] = jnp.concatenate([chip_sum[:-SUB], strip], axis=0).astype(jnp.bfloat16)

    @pl.when(exists)
    def _():
        over = swap(sent.at[1, head:], got.at[1, head:], 1, far)
        over.start()
        for at in range(2):
            pltpu.make_async_remote_copy(
                src_ref=sent.at[0, :head],
                dst_ref=early.at[at],
                send_sem=sems.at[6],
                recv_sem=sems.at[8 + at],
                device_id=far,
                device_id_type=MESH,
            ).wait_recv()
        over.wait()

    @pl.when(jnp.logical_not(exists))
    def _():
        got[1, head:] = jnp.zeros_like(got[1, head:])
        early[...] = jnp.zeros_like(early)

    theirs = jnp.concatenate(
        [early[0].astype(jnp.float32) + early[1].astype(jnp.float32), got[1, head:].astype(jnp.float32)], axis=0
    )
    pick = lambda at, here: jnp.where(
        row == 0, here, jnp.broadcast_to(theirs[-SUB : -SUB + 1, rest + at : rest + at + 1], basis.shape)
    )
    rank_mine, count_mine = pick(0, rank_here), pick(1, count_here)
    for at, lanes, piece in unfolded((chip_sum + theirs) * (1.0 / rows), rest):
        g_high, g_low = halves(piece)
        high[at, lanes] = g_high
        low[at, lanes] = g_low
    iterate(high, low, basis, count_mine, frames)
    index = lax.broadcasted_iota(jnp.int32, basis.shape, 0).astype(jnp.float32)
    kept = index < jnp.where(exists, rank_mine, 0.0)
    mine[...] = jnp.where(kept, basis[...], 0.0).astype(mine.dtype)
    pair = swap(mine, other, 2, partner)
    pair.start()

    @pl.when(before)
    def _():
        hand(0, down).wait_send()

    @pl.when(after)
    def _():
        hand(1, up).wait_send()

    pair.wait()
    own, theirs = mine[...], other[...]
    out[:size, :] = jnp.where(row == 0, own, theirs)
    out[size:, :] = jnp.where(row == 0, theirs, own)


def clutter_bases(echoes, start, rank, count, voxels):
    frames, size = start.shape
    wide = padded(frames + 2)
    chunks = 2
    hbm = pl.BlockSpec(memory_space=pltpu.HBM)
    vmem = pl.BlockSpec(memory_space=pltpu.VMEM)
    square = pltpu.VMEM((wide, wide), jnp.bfloat16)
    return pl.pallas_call(
        functools.partial(clutter_kernel, voxels, chunks),
        out_shape=[
            jax.ShapeDtypeStruct((2 * size, wide), jnp.bfloat16),
            jax.ShapeDtypeStruct(echoes.shape, echoes.dtype),
        ],
        in_specs=[hbm] * 2 + [pl.BlockSpec(memory_space=pltpu.SMEM)] * 2,
        out_specs=[vmem] * 2,
        scratch_shapes=[
            pltpu.VMEM((frames, wide), jnp.float32),
            pltpu.VMEM((2, 2 * frames - 3 * LANES // 2, LANES), jnp.bfloat16),
            pltpu.VMEM((2, 2 * frames - 3 * LANES // 2, LANES), jnp.bfloat16),
            pltpu.VMEM((2, (2 * frames - 3 * LANES // 2) // 32 * HEAD, LANES), jnp.bfloat16),
            square,
            square,
            pltpu.VMEM((size, wide), jnp.float32),
            pltpu.VMEM((size, wide), jnp.bfloat16),
            pltpu.VMEM((size, wide), jnp.bfloat16),
            pltpu.VMEM((size, frames), jnp.float32),
            pltpu.SMEM(rank.shape, jnp.int32),
            pltpu.SMEM(count.shape, jnp.int32),
            pltpu.SemaphoreType.DMA((3 + 4,)),
            pltpu.SemaphoreType.DMA((10,)),
        ],
        compiler_params=pltpu.CompilerParams(collective_id=0, has_side_effects=True, vmem_limit_bytes=GRANT),
        name="clutter",
    )(*(pltpu.with_memory_space_constraint(x, pltpu.HBM) for x in (echoes, start.T)), rank, count)


def project_kernel(span, frames, echoes, vectors, scale_y, scale_x, out):
    base = pl.program_id(0) * (echoes.shape[0] // scale_y.shape[0])
    chunk = scale_y.shape[0]
    q = vectors[:, :frames]
    for part in range(echoes.shape[0] // chunk):
        at = pl.ds(part * chunk, chunk)
        local = echoes[at, :]
        coeff = nt(local, q) * (scale_y[...] * scale_x[pl.ds(base + part, 1), :])
        clutter = jnp.dot(coeff.astype(jnp.bfloat16), q, preferred_element_type=jnp.float32)
        out[at, :] = (local.astype(jnp.float32) - clutter).astype(out.dtype)


def project(echoes, vectors, scale_y, scale_x):
    voxels, frames = echoes.shape
    span = scale_x.shape[0]
    steps = 4
    while span % steps:
        steps //= 2
    whole = lambda a: pl.BlockSpec(a.shape, lambda i: (0, 0))
    return pl.pallas_call(
        functools.partial(project_kernel, span, frames),
        out_shape=jax.ShapeDtypeStruct(echoes.shape, echoes.dtype),
        grid=(steps,),
        in_specs=[
            pl.BlockSpec((voxels // steps, frames), lambda i: (i, 0)),
            whole(vectors),
            whole(scale_y),
            whole(scale_x),
        ],
        out_specs=pl.BlockSpec((voxels // steps, frames), lambda i: (i, 0)),
        name="project",
    )(echoes, vectors, scale_y, scale_x)


def separate_kernel(groups, echoes, vectors, out, result, base, slope, stores):
    span, lines, depth, frames = echoes.shape
    size = vectors.shape[0] // 2
    col, cols = lax.axis_index("gy"), lax.axis_size("gy")
    part = lines // groups
    line = lambda i: pl.ds(i * part, part)
    writes = [pltpu.make_async_copy(result.at[:, line(i)], out.at[:, line(i)], stores.at[i]) for i in range(groups)]
    projector = lambda q: lax.dot_general(q, q, (((0,), (0,)), ((), ())), preferred_element_type=jnp.float32)
    after = projector(vectors[:size, :frames])
    before = projector(vectors[size:, :frames])
    base[...] = before
    slope[...] = after - before
    for i in range(groups):
        for y in range(i * part, i * part + part):
            share = (1.0 + y) / (1.0 + lines)
            share = jnp.where(col == 0, 1.0, jnp.where(col == cols - 1, 0.0, share))
            mixed = (base[...] + share * slope[...]).astype(jnp.bfloat16)
            block = echoes[:, y].reshape(span * depth, frames)
            clutter = jnp.dot(block, mixed, preferred_element_type=jnp.float32)
            rest = (block.astype(jnp.float32) - clutter).astype(out.dtype)
            result[:, y] = rest.reshape(span, depth, frames)
        writes[i].start()
    for copy in writes:
        copy.wait()


def separate(echoes, vectors):
    groups = 8
    frames = echoes.shape[-1]
    anywhere = pl.BlockSpec(memory_space=pl.ANY)
    square = pltpu.VMEM((frames, frames), jnp.float32)
    return pl.pallas_call(
        functools.partial(separate_kernel, groups),
        out_shape=jax.ShapeDtypeStruct(echoes.shape, echoes.dtype),
        in_specs=[pl.BlockSpec(memory_space=pltpu.VMEM)] * 2,
        out_specs=anywhere,
        scratch_shapes=[
            pltpu.VMEM(echoes.shape, echoes.dtype),
            square,
            square,
            pltpu.SemaphoreType.DMA((groups,)),
        ],
        compiler_params=pltpu.CompilerParams(vmem_limit_bytes=GRANT),
        name="separate",
    )(echoes, vectors)


def shares(span, index, count):
    offset = jnp.arange(span, dtype=jnp.float32)
    here = tent(offset, 2.0 * span) * (index <= count - 2).astype(jnp.float32)
    before = tent(offset + span, 2.0 * span) * (index >= 1).astype(jnp.float32)
    return here / (here + before), before / (here + before)


def body(echoes, start, ranks, counts):
    span, _, depth, frames = echoes.shape
    size = start.shape[1]
    row, col = lax.axis_index("gx"), lax.axis_index("gy")
    rows, cols = lax.axis_size("gx"), lax.axis_size("gy")
    flat = echoes.reshape(-1, frames)
    voxels = 4 * flat.shape[0]

    def sent(x, axis, route):
        return lax.ppermute(x, axis, route)

    def basis(total, count, rank, valid):
        return truncated_basis(
            total, start, count.reshape(1), rank.reshape(1), valid.astype(jnp.int32).reshape(1), float(voxels)
        )

    if rows == 2:
        vectors, held = clutter_bases(flat, start, ranks, counts, float(voxels))
        return separate(held.reshape(echoes.shape), vectors)
    back = lambda n: [(i, i - 1) for i in range(1, n)]
    ahead = lambda n: [(i - 1, i) for i in range(1, n)]
    gram = lax.dot_general(flat, flat, (((0,), (0,)), ((), ())), preferred_element_type=jnp.float32)
    pair = gram + sent(gram.astype(jnp.bfloat16), "gy", back(cols)).astype(jnp.float32)
    total = pair + sent(pair.astype(jnp.bfloat16), "gx", back(rows)).astype(jnp.float32)
    own = basis(total, counts[0, 0, 0], ranks[0, 0, 0], (row <= rows - 2) & (col <= cols - 2))
    left = sent(own, "gy", ahead(cols))
    paired = jnp.concatenate([own, left])
    vectors = jnp.concatenate([paired, sent(paired, "gx", ahead(rows))])
    y_here, y_before = shares(span, col, cols)
    x_here, x_before = shares(span, row, rows)
    scale_ys = [y_here, y_before, y_here, y_before]
    scale_xs = [x_here, x_here, x_before, x_before]
    wide = lambda parts: jnp.concatenate([jnp.broadcast_to(p[:, None], (span, size)) for p in parts], axis=1)
    scale_y = jnp.repeat(wide(scale_ys), depth, axis=0)
    return project(flat, vectors, scale_y, wide(scale_xs)).reshape(echoes.shape)


def solution(mesh):
    placed = (P("gx", "gy", None, None), P(), P("gx", "gy", None), P("gx", "gy", None))
    return jax.shard_map(
        body, mesh=mesh, in_specs=placed, out_specs=P("gx", "gy", None, None), check_vma=False
    )
```

```python
import functools

import jax
import jax.numpy as jnp
from jax import lax
from jax.experimental import pallas as pl
from jax.experimental.pallas import tpu as pltpu
from jax.sharding import PartitionSpec as P

BZ = 16
ITERS = 4
LANES = 128
SUB = 8
BLOCK = 16
HEAD = 16
GRANT = 16 << 20
MESH = pl.DeviceIdType.MESH


def tent(offset, span):
    inside = (offset >= 0.0) & (offset < span)
    return jnp.where(inside, 1.0 + jnp.minimum(offset, span - 1.0 - offset), 0.0)


def padded(size):
    return -(-size // LANES) * LANES


def row_of(tile, k):
    return jnp.broadcast_to(tile[k : k + 1, :], tile.shape)


def halves(x):
    high = x.astype(jnp.bfloat16)
    return high, (x - high.astype(jnp.float32)).astype(jnp.bfloat16)


def nt(a, b):
    return lax.dot_general(a, b, (((1,), (1,)), ((), ())), preferred_element_type=jnp.float32)


def product(high, low, other_high, other_low, dot):
    size = high.shape[0]
    both = dot(jnp.concatenate([high, low], axis=0), other_high)
    return both[:size] + both[size:] + dot(high, other_low)


def orthonormal_rows(inner, moved, spare):
    size = inner.shape[0]
    tiles, lanes = size // SUB, moved.shape[1] // LANES
    rows = [
        [moved[SUB * i : SUB * i + SUB, LANES * h : LANES * h + LANES] for h in range(lanes)] for i in range(tiles)
    ]
    place = lax.broadcasted_iota(jnp.int32, (SUB, LANES), 0)
    scales = [None] * tiles
    spread = lambda x: jnp.broadcast_to(x, (SUB, LANES))
    for k in range(size):
        own, at = k // SUB, k % SUB
        if k % BLOCK == 0:
            end = min(k + BLOCK, size)
            if k == 0:
                source, base = [inner[SUB * i : SUB * i + SUB] for i in range(tiles)], 0
            else:
                source, base = [r[spare // LANES] for r in rows], spare % LANES
            columns = {
                j: {i: spread(source[i][:, base + j : base + j + 1]) for i in range(j // SUB, tiles)}
                for j in range(k, end)
            }
            columns[k] = {i: jnp.where(place >= 0, c, 0.0) for i, c in columns[k].items()}
            pivot = row_of(columns[k][own], at)
        root = lax.rsqrt(pivot)
        scales[own] = root if at == 0 else jnp.where(place == at, root, scales[own])
        if k == size - 1:
            break
        inverse = root * root
        lines = {j: row_of(columns[k][j // SUB], j % SUB) for j in range(k + 1, end)}
        if k + 1 < end:
            pivot = row_of(columns[k + 1][(k + 1) // SUB], (k + 1) % SUB) - lines[k + 1] * lines[k + 1] * inverse
        factor = {i: c * inverse for i, c in columns[k].items()}
        factor[own] = jnp.where(place > at, factor[own], 0.0)
        for j in range(k + 1, end):
            columns[j] = {i: c - factor[i] * lines[j] for i, c in columns[j].items()}
        for h in reversed(range(lanes)):
            line = row_of(rows[own][h], at)
            for i in range(own if at < SUB - 1 else own + 1, tiles):
                rows[i][h] = rows[i][h] - factor[i] * line
    return jnp.concatenate(
        [jnp.concatenate([part * scales[i] for part in rows[i]], axis=1) for i in range(tiles)], axis=0
    )


def iterate(gram_high, gram_low, basis, count, frames):
    size, wide = basis.shape
    spare = -(-frames // 16) * 16
    own = slice(spare, spare + size)
    basis[...] = product(*halves(basis[...]), gram_high[...], gram_low[...], nt)
    lane = lax.broadcasted_iota(jnp.int32, basis.shape, 1)

    def turn(t):
        now = basis[...]
        high, low = halves(now)
        gram_high[own, :] = high
        gram_low[own, :] = low
        inner = product(high, low, high, low, nt)
        ahead = product(high, low, gram_high[...], gram_low[...], nt)
        last = t == ITERS - 1
        rows = jnp.where((lane < frames) & last, now, ahead)
        done = orthonormal_rows(inner, rows, spare)
        basis[...] = jnp.where(lane < frames, jnp.where((t + 1 < count) | last, done, now), 0.0)

    pl.loop(0, ITERS)(turn)


def subspace_kernel(rows, frames, count, rank, valid, gram, start, out, high, low, basis):
    high[...] = jnp.zeros_like(high)
    low[...] = jnp.zeros_like(low)
    basis[...] = jnp.zeros_like(basis)
    g_high, g_low = halves(gram[...] * (1.0 / rows))
    high[:frames, :frames] = g_high
    low[:frames, :frames] = g_low
    basis[:, :frames] = start[...]
    iterate(high, low, basis, count[0], frames)
    kept = lax.broadcasted_iota(jnp.int32, basis.shape, 0) < jnp.where(valid[0] > 0, rank[0], 0)
    out[...] = jnp.where(kept, basis[...], 0.0).astype(out.dtype)


def truncated_basis(gram, start, count, rank, valid, rows):
    frames, size = start.shape
    wide = padded(frames)
    smem = pl.BlockSpec(memory_space=pltpu.SMEM)
    vmem = pl.BlockSpec(memory_space=pltpu.VMEM)
    return pl.pallas_call(
        functools.partial(subspace_kernel, rows, frames),
        out_shape=jax.ShapeDtypeStruct((size, wide), jnp.bfloat16),
        in_specs=[smem, smem, smem, vmem, vmem],
        out_specs=vmem,
        scratch_shapes=[
            pltpu.VMEM((wide, wide), jnp.bfloat16),
            pltpu.VMEM((wide, wide), jnp.bfloat16),
            pltpu.VMEM((size, wide), jnp.float32),
        ],
        name="subspace",
    )(count, rank, valid, gram, start.T)


def folded(gram):
    half, rest = LANES // 2, gram.shape[0] - LANES
    corner = pltpu.roll(gram[:half, :LANES], half, 1)
    lane = lax.broadcasted_iota(jnp.int32, corner.shape, 1)
    return jnp.concatenate(
        [
            gram[half:LANES, :LANES],
            gram[LANES:, :LANES],
            jnp.where(lane < half, gram[LANES : LANES + half, LANES:], corner),
            gram[LANES + half :, LANES:],
        ],
        axis=0,
    )


def unfolded(packed, rest):
    half = LANES // 2
    lower, cross = packed[:half], packed[half : half + rest]
    square, strip = packed[half + rest : LANES + rest], packed[LANES + rest :]
    lane = lax.broadcasted_iota(jnp.int32, square.shape, 1)
    filled = lambda above, x, below: jnp.concatenate(
        [jnp.zeros((n, LANES), jnp.float32) if isinstance(n, int) else n for n in (above, x, below) if not isinstance(n, int) or n],
        axis=0,
    )
    upper = filled(half, lower, 0).T
    side = filled(half, strip, half - strip.shape[0]).T
    first = jnp.where(lane < half, pltpu.roll(square, half, 1), upper[:half])
    mixed = jnp.where(lane < half, square, jnp.where(lane < rest, side[:half], 0.0))
    tail = jnp.where(lax.broadcasted_iota(jnp.int32, strip.shape, 1) < rest, strip, 0.0)
    here, there = slice(0, LANES), slice(LANES, 2 * LANES)
    return (
        (slice(0, half), here, first),
        (slice(half, LANES), here, lower),
        (slice(LANES, LANES + rest), here, cross),
        (slice(0, LANES), there, filled(0, cross, LANES - rest).T),
        (slice(LANES, LANES + half), there, mixed),
        (slice(LANES + half, LANES + rest), there, tail),
    )


def clutter_kernel(
    rows, chunks, echoes_hbm, start_hbm, rank_hbm, count_hbm, out, echoes,
    gram, sent, got, early, high, low, basis, mine, other, start, rank, count, load, sems,
):
    row, col = lax.axis_index("gx"), lax.axis_index("gy")
    cols = lax.axis_size("gy")
    size, frames = start.shape
    wide = gram.shape[1]
    part = echoes.shape[0] // chunks
    pieces = echoes.shape[0] // (load.shape[0] - 3)
    slab = lambda i: pl.ds(i * pieces, pieces)
    loads = [
        pltpu.make_async_copy(echoes_hbm.at[slab(i)], echoes.at[slab(i)], load.at[3 + i])
        for i in range(load.shape[0] - 3)
    ]
    small = [
        pltpu.make_async_copy(start_hbm, start, load.at[2]),
    ]
    partner = (1 - row, col)
    side = 1 - 2 * row
    far = (1 - row, col + side)
    before, after = col >= 1, col + 1 < cols
    exists = jnp.where(row == 0, after, before)
    down, up = (0, col - 1), (1, col + 1)
    barrier = pltpu.get_barrier_semaphore()
    meet = lambda peer: pl.semaphore_signal(barrier, inc=1, device_id=peer, device_id_type=MESH)
    meet(partner)

    @pl.when(before)
    def _():
        meet(down)

    @pl.when(after)
    def _():
        meet(up)

    @pl.when(exists)
    def _():
        meet((row, col + side))

    for copy in loads + small:
        copy.start()

    def swap(source, target, at, peer):
        return pltpu.make_async_remote_copy(
            src_ref=source,
            dst_ref=target,
            send_sem=sems.at[2 * at],
            recv_sem=sems.at[2 * at + 1],
            device_id=peer,
            device_id_type=MESH,
        )

    high[...] = jnp.zeros_like(high)
    low[...] = jnp.zeros_like(low)
    basis[...] = jnp.zeros_like(basis)
    gram[...] = jnp.zeros_like(gram)
    total = None
    for i in range(chunks):
        for copy in loads[i * len(loads) // chunks : (i + 1) * len(loads) // chunks]:
            copy.wait()
        block = echoes[i * part : (i + 1) * part, :]
        term = lax.dot_general(block, block, (((0,), (0,)), ((), ())), preferred_element_type=jnp.float32)
        total = term if total is None else total + term
    for copy in small:
        copy.wait()
    basis[:, :frames] = start[...]
    gram[:, :frames] = total
    mine_sum = folded(gram)
    sent[0] = mine_sum.astype(jnp.bfloat16)

    pl.semaphore_wait(barrier, 1 + jnp.where(before, 1 + row, 0) + jnp.where(after, 2 - row, 0))
    chip = swap(sent.at[0], got.at[0], 0, partner)
    chip.start()
    head = early.shape[1]

    def hand(at, peer):
        return pltpu.make_async_remote_copy(
            src_ref=sent.at[0, :head],
            dst_ref=early.at[row],
            send_sem=sems.at[6 + at],
            recv_sem=sems.at[8 + row],
            device_id=peer,
            device_id_type=MESH,
        )

    @pl.when(before)
    def _():
        hand(0, down).start()

    @pl.when(after)
    def _():
        hand(1, up).start()

    chip.wait()
    chip_sum = mine_sum + got[0].astype(jnp.float32)
    rank_here = rank_hbm[0, 0, 0].astype(jnp.float32)
    count_here = count_hbm[0, 0, 0].astype(jnp.float32)
    rest = frames - LANES
    lane = lax.broadcasted_iota(jnp.int32, (SUB, LANES), 1)
    strip = jnp.where(lane == rest, rank_here, jnp.where(lane == rest + 1, count_here, chip_sum[-SUB:]))
    sent[1] = jnp.concatenate([chip_sum[:-SUB], strip], axis=0).astype(jnp.bfloat16)

    @pl.when(exists)
    def _():
        over = swap(sent.at[1, head:], got.at[1, head:], 1, far)
        over.start()
        for at in range(2):
            pltpu.make_async_remote_copy(
                src_ref=sent.at[0, :head],
                dst_ref=early.at[at],
                send_sem=sems.at[6],
                recv_sem=sems.at[8 + at],
                device_id=far,
                device_id_type=MESH,
            ).wait_recv()
        over.wait()

    @pl.when(jnp.logical_not(exists))
    def _():
        got[1, head:] = jnp.zeros_like(got[1, head:])
        early[...] = jnp.zeros_like(early)

    theirs = jnp.concatenate(
        [early[0].astype(jnp.float32) + early[1].astype(jnp.float32), got[1, head:].astype(jnp.float32)], axis=0
    )
    pick = lambda at, here: jnp.where(
        row == 0, here, jnp.broadcast_to(theirs[-SUB : -SUB + 1, rest + at : rest + at + 1], basis.shape)
    )
    rank_mine, count_mine = pick(0, rank_here), pick(1, count_here)
    for at, lanes, piece in unfolded((chip_sum + theirs) * (1.0 / rows), rest):
        g_high, g_low = halves(piece)
        high[at, lanes] = g_high
        low[at, lanes] = g_low
    iterate(high, low, basis, count_mine, frames)
    index = lax.broadcasted_iota(jnp.int32, basis.shape, 0).astype(jnp.float32)
    kept = index < jnp.where(exists, rank_mine, 0.0)
    mine[...] = jnp.where(kept, basis[...], 0.0).astype(mine.dtype)
    pair = swap(mine, other, 2, partner)
    pair.start()

    @pl.when(before)
    def _():
        hand(0, down).wait_send()

    @pl.when(after)
    def _():
        hand(1, up).wait_send()

    pair.wait()
    own, theirs = mine[...], other[...]
    out[:size, :] = jnp.where(row == 0, own, theirs)
    out[size:, :] = jnp.where(row == 0, theirs, own)


def clutter_bases(echoes, start, rank, count, voxels):
    frames, size = start.shape
    wide = padded(frames + 2)
    chunks = 2
    hbm = pl.BlockSpec(memory_space=pltpu.HBM)
    vmem = pl.BlockSpec(memory_space=pltpu.VMEM)
    square = pltpu.VMEM((wide, wide), jnp.bfloat16)
    return pl.pallas_call(
        functools.partial(clutter_kernel, voxels, chunks),
        out_shape=[
            jax.ShapeDtypeStruct((2 * size, wide), jnp.bfloat16),
            jax.ShapeDtypeStruct(echoes.shape, echoes.dtype),
        ],
        in_specs=[hbm] * 2 + [pl.BlockSpec(memory_space=pltpu.SMEM)] * 2,
        out_specs=[vmem] * 2,
        scratch_shapes=[
            pltpu.VMEM((frames, wide), jnp.float32),
            pltpu.VMEM((2, 2 * frames - 3 * LANES // 2, LANES), jnp.bfloat16),
            pltpu.VMEM((2, 2 * frames - 3 * LANES // 2, LANES), jnp.bfloat16),
            pltpu.VMEM((2, (2 * frames - 3 * LANES // 2) // 32 * HEAD, LANES), jnp.bfloat16),
            square,
            square,
            pltpu.VMEM((size, wide), jnp.float32),
            pltpu.VMEM((size, wide), jnp.bfloat16),
            pltpu.VMEM((size, wide), jnp.bfloat16),
            pltpu.VMEM((size, frames), jnp.float32),
            pltpu.SMEM(rank.shape, jnp.int32),
            pltpu.SMEM(count.shape, jnp.int32),
            pltpu.SemaphoreType.DMA((3 + 4,)),
            pltpu.SemaphoreType.DMA((10,)),
        ],
        compiler_params=pltpu.CompilerParams(collective_id=0, has_side_effects=True, vmem_limit_bytes=GRANT),
        name="clutter",
    )(*(pltpu.with_memory_space_constraint(x, pltpu.HBM) for x in (echoes, start.T)), rank, count)


def project_kernel(span, frames, echoes, vectors, scale_y, scale_x, out):
    base = pl.program_id(0) * (echoes.shape[0] // scale_y.shape[0])
    chunk = scale_y.shape[0]
    q = vectors[:, :frames]
    for part in range(echoes.shape[0] // chunk):
        at = pl.ds(part * chunk, chunk)
        local = echoes[at, :]
        coeff = nt(local, q) * (scale_y[...] * scale_x[pl.ds(base + part, 1), :])
        clutter = jnp.dot(coeff.astype(jnp.bfloat16), q, preferred_element_type=jnp.float32)
        out[at, :] = (local.astype(jnp.float32) - clutter).astype(out.dtype)


def project(echoes, vectors, scale_y, scale_x):
    voxels, frames = echoes.shape
    span = scale_x.shape[0]
    steps = 4
    while span % steps:
        steps //= 2
    whole = lambda a: pl.BlockSpec(a.shape, lambda i: (0, 0))
    return pl.pallas_call(
        functools.partial(project_kernel, span, frames),
        out_shape=jax.ShapeDtypeStruct(echoes.shape, echoes.dtype),
        grid=(steps,),
        in_specs=[
            pl.BlockSpec((voxels // steps, frames), lambda i: (i, 0)),
            whole(vectors),
            whole(scale_y),
            whole(scale_x),
        ],
        out_specs=pl.BlockSpec((voxels // steps, frames), lambda i: (i, 0)),
        name="project",
    )(echoes, vectors, scale_y, scale_x)


def separate_kernel(groups, echoes, vectors, out, result, base, slope, stores):
    span, lines, depth, frames = echoes.shape
    size = vectors.shape[0] // 2
    col, cols = lax.axis_index("gy"), lax.axis_size("gy")
    part = lines // groups
    line = lambda i: pl.ds(i * part, part)
    writes = [pltpu.make_async_copy(result.at[:, line(i)], out.at[:, line(i)], stores.at[i]) for i in range(groups)]
    projector = lambda q: lax.dot_general(q, q, (((0,), (0,)), ((), ())), preferred_element_type=jnp.float32)
    after = projector(vectors[:size, :frames])
    before = projector(vectors[size:, :frames])
    diagonal = lax.broadcasted_iota(jnp.int32, base.shape, 0) == lax.broadcasted_iota(jnp.int32, base.shape, 1)
    base[...] = jnp.where(diagonal, 1.0, 0.0) - before
    slope[...] = before - after
    for i in range(groups):
        for y in range(i * part, i * part + part):
            share = (1.0 + y) / (1.0 + lines)
            share = jnp.where(col == 0, 1.0, jnp.where(col == cols - 1, 0.0, share))
            mixed = (base[...] + share * slope[...]).astype(jnp.bfloat16)
            block = echoes[:, y].reshape(span * depth, frames)
            rest = jnp.dot(block, mixed, preferred_element_type=jnp.float32).astype(out.dtype)
            result[:, y] = rest.reshape(span, depth, frames)
        writes[i].start()
    for copy in writes:
        copy.wait()


def separate(echoes, vectors):
    groups = 8
    frames = echoes.shape[-1]
    anywhere = pl.BlockSpec(memory_space=pl.ANY)
    square = pltpu.VMEM((frames, frames), jnp.float32)
    return pl.pallas_call(
        functools.partial(separate_kernel, groups),
        out_shape=jax.ShapeDtypeStruct(echoes.shape, echoes.dtype),
        in_specs=[pl.BlockSpec(memory_space=pltpu.VMEM)] * 2,
        out_specs=anywhere,
        scratch_shapes=[
            pltpu.VMEM(echoes.shape, echoes.dtype),
            square,
            square,
            pltpu.SemaphoreType.DMA((groups,)),
        ],
        compiler_params=pltpu.CompilerParams(vmem_limit_bytes=GRANT),
        name="separate",
    )(echoes, vectors)


def shares(span, index, count):
    offset = jnp.arange(span, dtype=jnp.float32)
    here = tent(offset, 2.0 * span) * (index <= count - 2).astype(jnp.float32)
    before = tent(offset + span, 2.0 * span) * (index >= 1).astype(jnp.float32)
    return here / (here + before), before / (here + before)


def body(echoes, start, ranks, counts):
    span, _, depth, frames = echoes.shape
    size = start.shape[1]
    row, col = lax.axis_index("gx"), lax.axis_index("gy")
    rows, cols = lax.axis_size("gx"), lax.axis_size("gy")
    flat = echoes.reshape(-1, frames)
    voxels = 4 * flat.shape[0]

    def sent(x, axis, route):
        return lax.ppermute(x, axis, route)

    def basis(total, count, rank, valid):
        return truncated_basis(
            total, start, count.reshape(1), rank.reshape(1), valid.astype(jnp.int32).reshape(1), float(voxels)
        )

    if rows == 2:
        vectors, held = clutter_bases(flat, start, ranks, counts, float(voxels))
        return separate(held.reshape(echoes.shape), vectors)
    back = lambda n: [(i, i - 1) for i in range(1, n)]
    ahead = lambda n: [(i - 1, i) for i in range(1, n)]
    gram = lax.dot_general(flat, flat, (((0,), (0,)), ((), ())), preferred_element_type=jnp.float32)
    pair = gram + sent(gram.astype(jnp.bfloat16), "gy", back(cols)).astype(jnp.float32)
    total = pair + sent(pair.astype(jnp.bfloat16), "gx", back(rows)).astype(jnp.float32)
    own = basis(total, counts[0, 0, 0], ranks[0, 0, 0], (row <= rows - 2) & (col <= cols - 2))
    left = sent(own, "gy", ahead(cols))
    paired = jnp.concatenate([own, left])
    vectors = jnp.concatenate([paired, sent(paired, "gx", ahead(rows))])
    y_here, y_before = shares(span, col, cols)
    x_here, x_before = shares(span, row, rows)
    scale_ys = [y_here, y_before, y_here, y_before]
    scale_xs = [x_here, x_here, x_before, x_before]
    wide = lambda parts: jnp.concatenate([jnp.broadcast_to(p[:, None], (span, size)) for p in parts], axis=1)
    scale_y = jnp.repeat(wide(scale_ys), depth, axis=0)
    return project(flat, vectors, scale_y, wide(scale_xs)).reshape(echoes.shape)


def solution(mesh):
    placed = (P("gx", "gy", None, None), P(), P("gx", "gy", None), P("gx", "gy", None))
    return jax.shard_map(
        body, mesh=mesh, in_specs=placed, out_specs=P("gx", "gy", None, None), check_vma=False
    )
```
